32 devices in a mesh: gx: 8 (over z, x), gy: 4 (over y, core).
Axes of the slice: x: 2, y: 2, z: 4, core: 2. Of those that a mesh axis runs over, the one named last changes fastest.
Arguments:
- initial_guess_field: float32 [2, 2, 512, 2048], P(None, None, 'gx', 'gy'), may hold values from -18 to 18
- medium_label: int32 [512, 2048], P('gx', 'gy'), may hold values from 0 to 3
- principal_entry_addend: float32 [4, 2], replicated, may hold values from -0.5 to 0.8, as said below
- linearized_block_weight: float32 [25, 4, 2], replicated, may hold values from -1.25 to 1.25
- sample_abscissae: float32 [24, 2], replicated, may hold values from -1 to 1
- singularity_locations: float32 [24, 2], replicated, may hold values from -1 to 6, as said below
- basis_normalizers: float32 [24], replicated, may hold values from 0.8 to 1.6
- spectral_target: float32 [2], replicated, may hold values from -0.5 to 0.5
- quasi_periodic_phase: float32 [2, 2], replicated, may hold values from -3.140625 to 3.140625
Outputs:
- basis: float32 [2, 3, 2, 512, 2048], P(None, None, None, 'gx', 'gy')
- hessenberg: float32 [2, 2, 4, 3], replicated
The draws below stay inside these ranges and needn't reach their ends.
Inputs may be any that keep to these rules, and one draw needn't show every extreme that they name: `principal_entry_addend`: real parts lie in 0.2 to 0.8, imaginary parts in -0.5 to 0.5. `singularity_locations`: real parts lie in 3 to 6, imaginary parts in -1 to 1.
All inputs are finite; a program needn't handle non-finite values.
Results may differ from the reference program's by a relative error of at most 0.0003.
Values sent between devices are 32-bit elements; how exact they have to be, the bound alone decides.
No kernel may reach another device: no remote copies, remote signals or barrier semaphores. Data moves between devices by JAX's collectives and lax.ppermute only.
A program may use at most 128 MiB of HBM per device.

```python
import jax
import jax.numpy as jnp
from jax import lax

KPTS = 2
SAMPLE_TOTAL = 24
MATS = 4
STEPS = 3
SWEEPS = 4
BLOCKS = 25
NX = 512
NY = 2048


def draw_initial_guess_field(key, part):
    base_key = jax.random.fold_in(key, 37)
    row_share = jnp.arange(NX, dtype=jnp.float32) / max(NX - 1, 1)
    values = jax.random.truncated_normal(base_key, -6.0, 6.0, (KPTS, 2, NX, NY), jnp.float32)
    scale = 1.0 + 2.0 * row_share
    return values * scale[None, None, :, None]


def draw_principal_entry_addend(key, part):
    first_key, second_key = jax.random.split(jax.random.fold_in(key, 11))
    real_part = jax.random.uniform(first_key, (MATS,), jnp.float32, 0.2, 0.8)
    imag_part = jax.random.uniform(second_key, (MATS,), jnp.float32, -0.5, 0.5)
    return jnp.stack([real_part, imag_part], 1)


def draw_singularity_locations(key, part):
    first_key, second_key = jax.random.split(jax.random.fold_in(key, 23))
    real_part = jax.random.uniform(first_key, (SAMPLE_TOTAL,), jnp.float32, 3.0, 6.0)
    imag_part = jax.random.uniform(second_key, (SAMPLE_TOTAL,), jnp.float32, -1.0, 1.0)
    return jnp.stack([real_part, imag_part], 1)


def plant(drawn, rng, low, largest):
    longest = drawn.shape.index(max(drawn.shape))
    spots = []
    for shift in (0, 1):
        where = [jax.random.randint(jax.random.fold_in(rng, axis), (), 0, length) for axis, length in enumerate(drawn.shape)]
        where[longest] = (where[longest] + shift) % drawn.shape[longest]
        spots.append(tuple(where))
    return drawn.at[spots[0]].set(low).at[spots[1]].set(largest)


def bell_draw(key, shape, spread, limit, kind=jnp.bfloat16):
    array = spread * jax.random.normal(key, shape, jnp.float32)
    return jnp.clip(array, min=-limit, max=limit).astype(kind)


def setup_inputs(seed: int = 0) -> dict:
    key_of = jax.random.split(jax.random.key(seed), 10)
    initial_guess_field = draw_initial_guess_field(jax.random.fold_in(key_of[9], 71), 0)
    medium_label = plant(jax.random.randint(key_of[1], (NX, NY), 0, MATS), jax.random.fold_in(key_of[1], 1), 0, MATS - 1).astype(jnp.int32)
    principal_entry_addend = draw_principal_entry_addend(jax.random.fold_in(key_of[9], 71), 0)
    linearized_block_weight = bell_draw(key_of[3], (BLOCKS, MATS, 2), BLOCKS ** -0.5, 1.25, jnp.float32)
    sample_abscissae = jnp.clip(jax.random.uniform(key_of[4], (SAMPLE_TOTAL, 2), jnp.float32, -1.0, 1.0), -1.0, 1.0)
    singularity_locations = draw_singularity_locations(jax.random.fold_in(key_of[9], 71), 0)
    basis_normalizers = jnp.clip(jax.random.uniform(key_of[6], (SAMPLE_TOTAL,), jnp.float32, 0.8, 1.6), 0.8, 1.6)
    spectral_target = jnp.clip(jax.random.uniform(key_of[7], (2,), jnp.float32, -0.5, 0.5), -0.5, 0.5)
    quasi_periodic_phase = jnp.clip(jax.random.uniform(key_of[8], (KPTS, 2), jnp.float32, -3.140625, 3.140625), -3.140625, 3.140625)
    return {"initial_guess_field": initial_guess_field, "medium_label": medium_label, "principal_entry_addend": principal_entry_addend, "linearized_block_weight": linearized_block_weight, "sample_abscissae": sample_abscissae, "singularity_locations": singularity_locations, "basis_normalizers": basis_normalizers, "spectral_target": spectral_target, "quasi_periodic_phase": quasi_periodic_phase}


HIGHEST = lax.Precision.HIGHEST

def fraction_weights(sample_abscissae, singularity_locations, basis_normalizers, spectral_target):
    gap_real = spectral_target[0] - sample_abscissae[:, 0]
    gap_imag = spectral_target[1] - sample_abscissae[:, 1]
    pole_size = singularity_locations[:, 0] * singularity_locations[:, 0] + singularity_locations[:, 1] * singularity_locations[:, 1]
    quotient_inphase = (spectral_target[0] * singularity_locations[:, 0] + spectral_target[1] * singularity_locations[:, 1]) / pole_size
    quotient_quadrature = (spectral_target[1] * singularity_locations[:, 0] - spectral_target[0] * singularity_locations[:, 1]) / pole_size
    subordinate_inphase = basis_normalizers * (1.0 - quotient_inphase)
    subordinate_quadrature = -basis_normalizers * quotient_quadrature
    lower_size = subordinate_inphase * subordinate_inphase + subordinate_quadrature * subordinate_quadrature
    multiplier_inphase = (gap_real * subordinate_inphase + gap_imag * subordinate_quadrature) / lower_size
    multiplier_quadrature = (gap_imag * subordinate_inphase - gap_real * subordinate_quadrature) / lower_size
    return (multiplier_inphase, multiplier_quadrature)

def cell_inverse(onehot, principal_entry_addend):
    shifted = jnp.einsum('mxy,mc->cxy', onehot, principal_entry_addend, precision=HIGHEST)
    center = 4.0 + shifted[0]
    size_sq = center * center + shifted[1] * shifted[1]
    return jnp.stack([center / size_sq, -shifted[1] / size_sq])

def times_inverse(grid_field, inverse):
    real_part = grid_field[:, 0] * inverse[0] - grid_field[:, 1] * inverse[1]
    imag_part = grid_field[:, 0] * inverse[1] + grid_field[:, 1] * inverse[0]
    return jnp.stack([real_part, imag_part], 1)

def neighbours(padded):
    return padded[:, :, 2:, 1:-1] + padded[:, :, :-2, 1:-1] + padded[:, :, 1:-1, 2:] + padded[:, :, 1:-1, :-2]

def rotate(padded, angles, row_sign, column_sign):
    phase_angle = row_sign[None, :, None] * angles[:, 0][:, None, None] + column_sign[None, None, :] * angles[:, 1][:, None, None]
    cosine = jnp.cos(phase_angle)
    sine_part = jnp.sin(phase_angle)
    real_part = padded[:, 0] * cosine - padded[:, 1] * sine_part
    imag_part = padded[:, 0] * sine_part + padded[:, 1] * cosine
    return jnp.stack([real_part, imag_part], 1)

def twist(padded, angles, margin):
    row_count = padded.shape[2]
    column_count = padded.shape[3]
    row_positions = jnp.arange(row_count)
    column_positions = jnp.arange(column_count)
    row_sign = jnp.where(row_positions < margin, -1.0, 0.0) + jnp.where(row_positions >= row_count - margin, 1.0, 0.0)
    column_sign = jnp.where(column_positions < margin, -1.0, 0.0) + jnp.where(column_positions >= column_count - margin, 1.0, 0.0)
    return rotate(padded, angles, row_sign.astype(jnp.float32), column_sign.astype(jnp.float32))

def relax_jacobi(source, inverse, angles):
    solved = times_inverse(source, inverse)
    for repeat in range(SWEEPS):
        padded = jnp.pad(solved, ((0, 0), (0, 0), (1, 1), (1, 1)), mode='wrap')
        padded = twist(padded, angles, 1)
        solved = times_inverse(source + neighbours(padded), inverse)
    return solved

def right_side(vectors_now, current, linearized_block_weight, onehot):
    mixing_real = jnp.einsum('bm,kbc->kmc', linearized_block_weight[:, :, 0], current[:, :, 0], precision=HIGHEST) - jnp.einsum('bm,kbc->kmc', linearized_block_weight[:, :, 1], current[:, :, 1], precision=HIGHEST)
    mixing_imag = jnp.einsum('bm,kbc->kmc', linearized_block_weight[:, :, 0], current[:, :, 1], precision=HIGHEST) + jnp.einsum('bm,kbc->kmc', linearized_block_weight[:, :, 1], current[:, :, 0], precision=HIGHEST)
    cell_real = jnp.einsum('kmc,mxy->kcxy', mixing_real, onehot, precision=HIGHEST)
    cell_imag = jnp.einsum('kmc,mxy->kcxy', mixing_imag, onehot, precision=HIGHEST)
    real_part = lax.optimization_barrier(jnp.sum(cell_real * vectors_now[:, :, 0] - cell_imag * vectors_now[:, :, 1], axis=1))
    imag_part = lax.optimization_barrier(jnp.sum(cell_real * vectors_now[:, :, 1] + cell_imag * vectors_now[:, :, 0], axis=1))
    return jnp.stack([real_part, imag_part], 1)

def grid_inner(vectors_now, grid_field):
    inner_real = jnp.einsum('kcxy,kxy->kc', vectors_now[:, :, 0], grid_field[:, 0], precision=HIGHEST) + jnp.einsum('kcxy,kxy->kc', vectors_now[:, :, 1], grid_field[:, 1], precision=HIGHEST)
    inner_imag = jnp.einsum('kcxy,kxy->kc', vectors_now[:, :, 0], grid_field[:, 1], precision=HIGHEST) - jnp.einsum('kcxy,kxy->kc', vectors_now[:, :, 1], grid_field[:, 0], precision=HIGHEST)
    return (inner_real, inner_imag)

def grid_remove(vectors_now, grid_field, inner_real, inner_imag):
    real_part = grid_field[:, 0] - (jnp.einsum('kc,kcxy->kxy', inner_real, vectors_now[:, :, 0], precision=HIGHEST) - jnp.einsum('kc,kcxy->kxy', inner_imag, vectors_now[:, :, 1], precision=HIGHEST))
    imag_part = grid_field[:, 1] - (jnp.einsum('kc,kcxy->kxy', inner_real, vectors_now[:, :, 1], precision=HIGHEST) + jnp.einsum('kc,kcxy->kxy', inner_imag, vectors_now[:, :, 0], precision=HIGHEST))
    return jnp.stack([real_part, imag_part], 1)

def block_chain(coords_real, coords_imag, current_full, multiplier_inphase, multiplier_quadrature):
    blockwise = [jnp.stack([coords_real, coords_imag], 1)]
    for block_id in range(current_full.shape[1] - 1):
        previous = blockwise[-1]
        real_part = multiplier_inphase[block_id] * previous[:, 0] - multiplier_quadrature[block_id] * previous[:, 1] + current_full[:, block_id + 1, 0]
        imag_part = multiplier_inphase[block_id] * previous[:, 1] + multiplier_quadrature[block_id] * previous[:, 0] + current_full[:, block_id + 1, 1]
        blockwise.append(jnp.stack([real_part, imag_part], 1))
    return jnp.stack(blockwise, 1)

def level_inner(older, newer):
    inner_real = jnp.einsum('kcbr,kbr->kc', older[:, :, :, 0], newer[:, :, 0], precision=HIGHEST) + jnp.einsum('kcbr,kbr->kc', older[:, :, :, 1], newer[:, :, 1], precision=HIGHEST)
    inner_imag = jnp.einsum('kcbr,kbr->kc', older[:, :, :, 0], newer[:, :, 1], precision=HIGHEST) - jnp.einsum('kcbr,kbr->kc', older[:, :, :, 1], newer[:, :, 0], precision=HIGHEST)
    return (inner_real, inner_imag)

def level_remove(older, newer, inner_real, inner_imag):
    real_part = newer[:, :, 0] - (jnp.einsum('kc,kcbr->kbr', inner_real, older[:, :, :, 0], precision=HIGHEST) - jnp.einsum('kc,kcbr->kbr', inner_imag, older[:, :, :, 1], precision=HIGHEST))
    imag_part = newer[:, :, 1] - (jnp.einsum('kc,kcbr->kbr', inner_real, older[:, :, :, 1], precision=HIGHEST) + jnp.einsum('kc,kcbr->kbr', inner_imag, older[:, :, :, 0], precision=HIGHEST))
    return jnp.stack([real_part, imag_part], 2)

def level_step(coeffs, hessen, blockwise, active, section_id):
    older = coeffs[:, :active]
    first_real, first_imag = level_inner(older, blockwise)
    orthog_once = level_remove(older, blockwise, first_real, first_imag)
    second_real, second_imag = level_inner(older, orthog_once)
    orthog_twice = level_remove(older, orthog_once, second_real, second_imag)
    length = jnp.sqrt(lax.optimization_barrier(jnp.sum(orthog_twice * orthog_twice, axis=(1, 2, 3))))
    coeffs = coeffs.at[:, active].set(orthog_twice / length[:, None, None, None])
    hessen = hessen.at[:, 0, :active, section_id].set(first_real + second_real)
    hessen = hessen.at[:, 1, :active, section_id].set(first_imag + second_imag)
    hessen = hessen.at[:, 0, active, section_id].set(length)
    return (coeffs, hessen)

def krylov(initial_guess_field, angles, onehot, inverse, linearized_block_weight, multiplier_inphase, multiplier_quadrature):
    points = initial_guess_field.shape[0]
    blocks = linearized_block_weight.shape[0]
    rank_count = STEPS + 1
    scale_start = jnp.sqrt(lax.optimization_barrier(jnp.sum(initial_guess_field * initial_guess_field, axis=(1, 2, 3))))
    vectors = [initial_guess_field / scale_start[:, None, None, None]]
    coeffs = jnp.zeros((points, rank_count, blocks, 2, rank_count), jnp.float32).at[:, 0, 0, 0, 0].set(1.0)
    hessen = jnp.zeros((points, 2, rank_count, STEPS), jnp.float32)
    for section_id in range(STEPS):
        active = section_id + 1
        vectors_now = jnp.stack(vectors, 1)
        source = right_side(vectors_now, coeffs[:, section_id, :, :, :active], linearized_block_weight, onehot)
        solved = relax_jacobi(source, inverse, angles)
        inner_real, inner_imag = grid_inner(vectors_now, solved)
        orthog_once = grid_remove(vectors_now, solved, inner_real, inner_imag)
        length = jnp.sqrt(lax.optimization_barrier(jnp.sum(orthog_once * orthog_once, axis=(1, 2, 3))))
        vectors.append(orthog_once / length[:, None, None, None])
        coords_real = jnp.zeros((points, rank_count), jnp.float32).at[:, :active].set(inner_real).at[:, active].set(length)
        coords_imag = jnp.zeros((points, rank_count), jnp.float32).at[:, :active].set(inner_imag)
        blockwise = block_chain(coords_real, coords_imag, coeffs[:, section_id], multiplier_inphase, multiplier_quadrature)
        coeffs, hessen = level_step(coeffs, hessen, blockwise, active, section_id)
    return (jnp.stack(vectors[1:], 1), hessen)

def reference(initial_guess_field, medium_label, principal_entry_addend, linearized_block_weight, sample_abscissae, singularity_locations, basis_normalizers, spectral_target, quasi_periodic_phase):
    materials = principal_entry_addend.shape[0]
    onehot = (medium_label.astype(jnp.int32)[None] == jnp.arange(materials, dtype=jnp.int32)[:, None, None]).astype(jnp.float32)
    inverse = cell_inverse(onehot, principal_entry_addend)
    multiplier_inphase, multiplier_quadrature = fraction_weights(sample_abscissae, singularity_locations, basis_normalizers, spectral_target)

    def solve_point(point_data):
        grid_field, angles = point_data
        found, hessen = krylov(grid_field[None], angles[None], onehot, inverse, linearized_block_weight, multiplier_inphase, multiplier_quadrature)
        return (found[0], hessen[0])
    basis, hessenberg = lax.map(solve_point, (initial_guess_field, quasi_periodic_phase))
    return (basis, hessenberg)
```

```python
import functools

import jax
import jax.numpy as jnp
from jax import lax
from jax.experimental import pallas as pl
from jax.experimental.pallas import tpu as pltpu
from jax.sharding import PartitionSpec as P

STEPS = 3
SWEEPS = 4
HALO = STEPS * SWEEPS
LANES = 128
SUB = 8
SLOT = 16
F32 = jnp.float32
VMEM = pl.BlockSpec(memory_space=pltpu.VMEM)
SMEM = pl.BlockSpec(memory_space=pltpu.SMEM)
ANY = pl.BlockSpec(memory_space=pl.ANY)
MIB = 1024 * 1024


def even(axis):
    return lax.rem(lax.axis_index(axis), 2) == 0


def swap_near(axis):
    return [(i, i ^ 1) for i in range(lax.axis_size(axis))]


def swap_far(axis):
    n = lax.axis_size(axis)
    return [(i, (i + 1) % n if i % 2 else (i - 1) % n) for i in range(n)]


def cmul(a, b):
    return (a[0] * b[0] - a[1] * b[1], a[0] * b[1] + a[1] * b[0])


def cadd(a, b):
    return (a[0] + b[0], a[1] + b[1])


def csub(a, b):
    return (a[0] - b[0], a[1] - b[1])


def conj_mul(a, b):
    return (a[0] * b[0] + a[1] * b[1], a[0] * b[1] - a[1] * b[0])


def pack_rows(z_ref, m_ref, near_ref, far_ref):
    points, _, rows, _ = z_ref.shape
    is_even = even("gx")
    for plane in range(2 * points + 1):
        if plane < 2 * points:
            top = z_ref[plane // 2, plane % 2, 0:HALO, :]
            bottom = z_ref[plane // 2, plane % 2, rows - HALO : rows, :]
        else:
            top = m_ref[0:HALO, :].astype(F32)
            bottom = m_ref[rows - HALO : rows, :].astype(F32)
        span = slice(plane * HALO, (plane + 1) * HALO)
        near_ref[span, :] = jnp.where(is_even, bottom, top)
        far_ref[span, :] = jnp.where(is_even, top, bottom)


def params(a_ref, w_ref, node_ref, pole_ref, scale_ref, target_ref, phase_ref,
           table_ref, trig_ref, chain_ref, size_ref):
    shape = (SUB, LANES)

    def splat(value):
        return jnp.full(shape, value, F32)

    mats = a_ref.shape[0]
    totals = node_ref.shape[0]
    target = (splat(target_ref[0]), splat(target_ref[1]))
    steps = []
    for j in range(totals):
        gap = csub(target, (splat(node_ref[j, 0]), splat(node_ref[j, 1])))
        pole = (splat(pole_ref[j, 0]), splat(pole_ref[j, 1]))
        pole_size = pole[0] * pole[0] + pole[1] * pole[1]
        quotient = conj_mul(pole, target)
        quotient = (quotient[0] / pole_size, quotient[1] / pole_size)
        scale = splat(scale_ref[j])
        lower = (scale * (1.0 - quotient[0]), -scale * quotient[1])
        size = lower[0] * lower[0] + lower[1] * lower[1]
        factor = conj_mul(lower, gap)
        steps.append((factor[0] / size, factor[1] / size))
    zero = jnp.zeros(shape, F32)
    power = (splat(1.0), zero)
    size = splat(1.0)
    sums = [zero[:mats, :2]] * 4
    for b in range(totals + 1):
        if b > 0:
            power = cmul(power, steps[b - 1])
            size = size + power[0] * power[0] + power[1] * power[1]
        w = w_ref[b]
        pr = power[0][:mats, :2]
        pi = power[1][:mats, :2]
        sums[0] = sums[0] + w * pr
        sums[1] = sums[1] + w * pi
        sums[2] = sums[2] + float(b) * (w * pr)
        sums[3] = sums[3] + float(b) * (w * pi)
    gamma = jnp.sqrt(size)
    size_ref[...] = gamma

    def full(value):
        return jnp.broadcast_to(value, shape)

    for m in range(mats):
        center = 4.0 + splat(a_ref[m, 0])
        side = splat(a_ref[m, 1])
        lower = center * center + side * side
        inverse = (center / lower, -side / lower)
        first = (full(w_ref[0, m : m + 1, 0:1]), full(w_ref[0, m : m + 1, 1:2]))
        parts = [[full(s[m : m + 1, c : c + 1]) for c in range(2)] for s in sums]
        a_weight = (parts[0][0] - parts[1][1], parts[0][1] + parts[1][0])
        b_weight = (parts[2][0] - parts[3][1], parts[2][1] + parts[3][0])
        a_weight = (a_weight[0] / gamma, a_weight[1] / gamma)
        b_weight = (b_weight[0] / gamma / gamma, b_weight[1] / gamma / gamma)
        entries = (inverse, cmul(inverse, first), cmul(inverse, a_weight), cmul(inverse, b_weight))
        for e, (re, im) in enumerate(entries):
            table_ref[2 * e, m] = re
            table_ref[2 * e + 1, m] = im
    for k in range(phase_ref.shape[0]):
        for axis in range(2):
            angle = splat(phase_ref[k, axis])
            trig_ref[k, axis, 0] = jnp.cos(angle)
            trig_ref[k, axis, 1] = jnp.sin(angle)
    depth = chain_ref.shape[2]
    row = lax.broadcasted_iota(jnp.int32, shape, 0)
    tiles = [[], []]
    for c in range(2):
        for t in range(depth // SUB):
            value = zero
            for r in range(SUB):
                b = t * SUB + r
                if 1 <= b <= totals:
                    value = jnp.where(row == r, steps[b - 1][c], value)
            tiles[c].append(value)
    step = tuple(jnp.concatenate(tile, 0) for tile in tiles)
    for s in range(chain_ref.shape[0]):
        chain_ref[s, 0] = step[0]
        chain_ref[s, 1] = step[1]
        moved = (pltpu.roll(step[0], 1 << s, 0), pltpu.roll(step[1], 1 << s, 0))
        step = cmul(step, moved)


def pack_columns(z_ref, m_ref, near_ref, far_ref, trig_ref, full_ref, near_out, far_out):
    points, _, rows, columns = z_ref.shape
    tiles = columns // LANES
    planes = 2 * points + 1
    total = rows + 2 * HALO
    is_even = even("gx")
    first = lax.axis_index("gx") == 0
    last = lax.axis_index("gx") == lax.axis_size("gx") - 1
    row = lax.broadcasted_iota(jnp.int32, (2 * HALO, LANES), 0)
    for plane in range(planes):
        span = slice(plane * HALO, (plane + 1) * HALO)
        for t in range(tiles):
            lanes = slice(t * LANES, (t + 1) * LANES)
            if plane < 2 * points:
                full_ref[plane, t, 0:rows, :] = z_ref[plane // 2, plane % 2, :, lanes]
            else:
                full_ref[plane, t, 0:rows, :] = m_ref[:, lanes].astype(F32)
            near = near_ref[span, lanes]
            far = far_ref[span, lanes]
            full_ref[plane, t, rows : rows + HALO, :] = jnp.where(is_even, near, far)
            full_ref[plane, t, rows + HALO : total, :] = jnp.where(is_even, far, near)
    for k in range(points):
        cosine = trig_ref[k, 0, 0][0:1, :]
        sine = trig_ref[k, 0, 1][0:1, :]
        low = row < HALO
        edge = jnp.where(low, last.astype(F32), first.astype(F32))
        co = jnp.where(edge > 0.5, cosine, 1.0)
        si = jnp.where(edge > 0.5, jnp.where(low, sine, -sine), 0.0)
        for t in range(tiles):
            re = full_ref[2 * k, t, rows:total, :]
            im = full_ref[2 * k + 1, t, rows:total, :]
            full_ref[2 * k, t, rows:total, :] = re * co - im * si
            full_ref[2 * k + 1, t, rows:total, :] = re * si + im * co
    y_even = even("gy")
    lane = lax.broadcasted_iota(jnp.int32, (total, LANES), 1)
    near_acc = jnp.zeros((total, LANES), F32)
    far_acc = jnp.zeros((total, LANES), F32)
    for plane in range(planes):
        left = full_ref[plane, 0]
        right = full_ref[plane, tiles - 1]
        base = plane * SLOT
        keep = (lane >= base) & (lane < base + HALO)
        to_left = jnp.int32(base)
        to_right = jnp.int32((base + HALO) % LANES)
        near = pltpu.roll(jnp.where(y_even, right, left), jnp.where(y_even, to_right, to_left), 1)
        far = pltpu.roll(jnp.where(y_even, left, right), jnp.where(y_even, to_left, to_right), 1)
        near_acc = jnp.where(keep, near, near_acc)
        far_acc = jnp.where(keep, far, far_acc)
    near_out[...] = near_acc
    far_out[...] = far_acc


def solve(full_ref, near_ref, far_ref, table_ref, trig_ref, out_ref, gram_ref,
          halo_ref, cell_ref, b_ref, x_ref, keep_ref):
    planes, tiles, total, _ = full_ref.shape
    points = planes // 2
    rows = out_ref.shape[4]
    mats = table_ref.shape[1]
    count = total // SUB
    y_even = even("gy")
    first = lax.axis_index("gy") == 0
    last = lax.axis_index("gy") == lax.axis_size("gy") - 1

    lane = lax.broadcasted_iota(jnp.int32, (total, LANES), 1)
    right_src = jnp.where(y_even, near_ref[...], far_ref[...])
    left_src = jnp.where(y_even, far_ref[...], near_ref[...])
    is_right = lane < HALO
    is_left = lane >= LANES - HALO
    for plane in range(planes):
        right = pltpu.roll(right_src, (LANES - plane * SLOT) % LANES, 1)
        left = pltpu.roll(left_src, (LANES - HALO - plane * SLOT) % LANES, 1)
        halo_ref[plane] = jnp.where(is_right, right, jnp.where(is_left, left, 0.0))
    edge = jnp.where(is_right, last.astype(F32), jnp.where(is_left, first.astype(F32), 0.0))
    for k in range(points):
        cosine = trig_ref[k, 1, 0][0:1, :]
        sine = trig_ref[k, 1, 1][0:1, :]
        co = jnp.where(edge > 0.5, cosine, 1.0)
        si = jnp.where(edge > 0.5, jnp.where(is_right, sine, -sine), 0.0)
        re = halo_ref[2 * k]
        im = halo_ref[2 * k + 1]
        halo_ref[2 * k] = re * co - im * si
        halo_ref[2 * k + 1] = re * si + im * co

    def rows_of(plane, t, v):
        span = pl.ds(v, SUB, stride=count)
        if t < tiles:
            return full_ref[plane, t, span, :]
        return halo_ref[plane, span, :]

    for t in range(tiles + 1):
        for v in range(count):
            label = rows_of(planes - 1, t, v)
            picks = [label == float(m) for m in range(1, mats)]

            def pick(e):
                value = table_ref[e, 0]
                for m in range(1, mats):
                    value = jnp.where(picks[m - 1], table_ref[e, m], value)
                return value

            for e in (0, 1):
                cell_ref[e, t, v] = pick(e)
            for e in (4, 5, 6, 7):
                cell_ref[e - 2, t, v] = pick(e)
            weight = (pick(2), pick(3))
            for k in range(points):
                z = (rows_of(2 * k, t, v), rows_of(2 * k + 1, t, v))
                for c, value in enumerate(cmul(weight, z)):
                    b_ref[k, c, t, v] = value
                    x_ref[0, k, c, t, v] = value

    lane8 = lax.broadcasted_iota(jnp.int32, (SUB, LANES), 1)
    at_first = lane8 == 0
    at_last = lane8 == LANES - 1

    def sweep(i, carry):
        src = lax.rem(i, 2)
        dst = 1 - src
        for k in range(points):
            for v in range(count):
                sides = []
                for c in range(2):
                    mine = [x_ref[src, k, c, t, v] for t in range(tiles + 1)]
                    ahead = [pltpu.roll(value, 1, 1) for value in mine]
                    behind = [pltpu.roll(value, LANES - 1, 1) for value in mine]
                    side = []
                    for t in range(tiles + 1):
                        one = jnp.where(at_first, ahead[t - 1], ahead[t])
                        two = jnp.where(at_last, behind[(t + 1) % (tiles + 1)], behind[t])
                        side.append(one + two)
                    sides.append(side)
                for t in range(tiles + 1):
                    n = []
                    for c in range(2):
                        if v > 0:
                            up = x_ref[src, k, c, t, v - 1]
                        else:
                            up = pltpu.roll(x_ref[src, k, c, t, count - 1], 1, 0)
                        if v < count - 1:
                            down = x_ref[src, k, c, t, v + 1]
                        else:
                            down = pltpu.roll(x_ref[src, k, c, t, 0], SUB - 1, 0)
                        n.append(sides[c][t] + (up + down))
                    inverse = (cell_ref[0, t, v], cell_ref[1, t, v])
                    n = cmul(inverse, n)
                    for c in range(2):
                        x_ref[dst, k, c, t, v] = b_ref[k, c, t, v] + n[c]
        return carry

    for s in range(STEPS):
        lax.fori_loop(0, SWEEPS, sweep, 0)
        final = SWEEPS % 2
        for k in range(points):
            for t in range(tiles + 1):
                for v in range(count):
                    y = (x_ref[final, k, 0, t, v], x_ref[final, k, 1, t, v])
                    if t < tiles:
                        for c in range(2):
                            out_ref[s, k, c, t, pl.ds(v, SUB, stride=count), :] = y[c]
                    if s < STEPS - 1:
                        b = cmul((cell_ref[2, t, v], cell_ref[3, t, v]), y)
                        if s == 0:
                            keep = cmul((cell_ref[4, t, v], cell_ref[5, t, v]), y)
                            for c in range(2):
                                keep_ref[k, c, t, v] = keep[c]
                        else:
                            b = cadd(b, (keep_ref[k, 0, t, v], keep_ref[k, 1, t, v]))
                        for c in range(2):
                            b_ref[k, c, t, v] = b[c]
                            x_ref[0, k, c, t, v] = b[c]

    rows = total - 2 * HALO
    names = STEPS + 1
    zero = jnp.zeros((SUB, LANES), F32)
    line = jnp.zeros((1, LANES), F32)
    lane1 = lax.broadcasted_iota(jnp.int32, (1, LANES), 1)
    entries = [(i, j) for i in range(names) for j in range(i, names)]
    for k in range(points):

        def gather(r, accs):
            accs = list(accs)
            span = pl.ds(pl.multiple_of(r * SUB, SUB), SUB)
            for t in range(tiles):
                fields = [(full_ref[2 * k, t, span, :], full_ref[2 * k + 1, t, span, :])]
                for s in range(STEPS):
                    fields.append((out_ref[s, k, 0, t, span, :], out_ref[s, k, 1, t, span, :]))
                at = 0
                for i, j in entries:
                    if i == j:
                        a = fields[i]
                        accs[at] = accs[at] + (a[0] * a[0] + a[1] * a[1])
                        at += 1
                    else:
                        product = conj_mul(fields[i], fields[j])
                        accs[at] = accs[at] + product[0]
                        accs[at + 1] = accs[at + 1] + product[1]
                        at += 2
            return tuple(accs)

        accs = lax.fori_loop(0, rows // SUB, gather, (zero,) * (names * names))
        for e, acc in enumerate(accs):
            value = jnp.sum(jnp.sum(acc, axis=0, keepdims=True), axis=1, keepdims=True)
            line = jnp.where(lane1 == k * names * names + e, value, line)
    gram_ref[...] = jnp.broadcast_to(line[None], gram_ref.shape)


def finish(full_ref, out_ref, part_ref, chain_ref, size_ref, basis_ref, hess_ref, done_ref, sem):
    planes, tiles, total, _ = full_ref.shape
    points = planes // 2
    rows = total - 2 * HALO
    names = STEPS + 1
    shape = (SUB, LANES)
    line = jnp.sum(part_ref[:, 0, :], axis=0, keepdims=True)
    uppers = []
    inverses = []
    copies = []
    for k in range(points):
        base = k * names * names
        gram = {}
        at = base
        for i in range(names):
            for j in range(i, names):
                width = 1 if i == j else 2
                gram[i, j] = tuple(
                    jnp.broadcast_to(line[:, at + c : at + c + 1], shape) for c in range(width)
                )
                at += width
        upper = {}
        inv = []
        for i in range(names):
            pivot = gram[i, i][0]
            for l in range(i):
                pivot = pivot - (upper[l, i][0] * upper[l, i][0] + upper[l, i][1] * upper[l, i][1])
            root = jnp.sqrt(pivot)
            upper[i, i] = root
            inv.append(1.0 / root)
            for j in range(i + 1, names):
                value = gram[i, j]
                for l in range(i):
                    value = csub(value, conj_mul(upper[l, i], upper[l, j]))
                upper[i, j] = (value[0] * inv[i], value[1] * inv[i])
        uppers.append(upper)
        inverses.append(inv)

        def combine(r, carry):
            span = pl.ds(pl.multiple_of(r * SUB, SUB), SUB)
            for t in range(tiles):
                lanes = slice(t * LANES, (t + 1) * LANES)
                fields = [(full_ref[2 * k, t, span, :], full_ref[2 * k + 1, t, span, :])]
                for s in range(STEPS):
                    fields.append((out_ref[s, k, 0, t, span, :], out_ref[s, k, 1, t, span, :]))
                found = []
                for i in range(names):
                    value = fields[i]
                    for l in range(i):
                        value = csub(value, cmul(upper[l, i], found[l]))
                    value = (value[0] * inv[i], value[1] * inv[i])
                    found.append(value)
                    if i > 0:
                        done_ref[k, i - 1, 0, span, lanes] = value[0]
                        done_ref[k, i - 1, 1, span, lanes] = value[1]
            return carry

        lax.fori_loop(0, rows // SUB, combine, 0)
        copy = pltpu.make_async_copy(done_ref.at[k], basis_ref.at[k], sem.at[k])
        copy.start()
        copies.append(copy)

    lane = lax.broadcasted_iota(jnp.int32, shape, 1)

    def mixed(pick):
        value = pick(0)
        for k in range(1, points):
            value = jnp.where(lane == k, pick(k), value)
        return value

    gamma = size_ref[...]
    inv0 = mixed(lambda k: inverses[k][0])
    column = []
    for j in range(1, names):
        entry = []
        for i in range(j):
            entry.append(tuple(mixed(lambda k: uppers[k][i, j][c]) * inv0 for c in range(2)))
        entry.append((mixed(lambda k: uppers[k][j, j]) * inv0, jnp.zeros(shape, F32)))
        column.append(entry)

    depth = chain_ref.shape[2]
    row = lax.broadcasted_iota(jnp.int32, (depth, LANES), 0)
    tall = lambda value: jnp.broadcast_to(value[0:1], (depth, LANES))
    nil = jnp.zeros((depth, LANES), F32)
    at_top = row == 0
    basis_u = [[(jnp.where(at_top, 1.0, 0.0), nil)]]
    hess = {}
    coords = []
    mus = []
    for k in range(STEPS):
        active = k + 1
        if k == 0:
            found = column[0]
        elif k == 1:
            found = []
            for i in range(3):
                value = (column[1][i][0] * gamma, column[1][i][1] * gamma)
                if i < 2:
                    value = csub(value, cmul(hess[0, 0], coords[0][i]))
                found.append((value[0] / mus[0], value[1] / mus[0]))
        else:
            found = []
            scale = gamma / mus[0]
            for i in range(4):
                value = (column[2][i][0] * gamma, column[2][i][1] * gamma)
                if i < 3:
                    value = csub(value, cmul(hess[0, 0], column[1][i]))
                value = (value[0] * scale, value[1] * scale)
                if i < 2:
                    value = csub(value, cmul(hess[0, 1], coords[0][i]))
                if i < 3:
                    value = csub(value, cmul(hess[1, 1], coords[1][i]))
                found.append((value[0] / mus[1], value[1] / mus[1]))
        coords.append(found)
        current = basis_u[k]
        x = []
        for i in range(active + 1):
            old = current[i] if i < len(current) else (nil, nil)
            value = tuple(jnp.where(at_top, tall(found[i][c]), old[c]) for c in range(2))
            for s in range(chain_ref.shape[0]):
                step = (chain_ref[s, 0], chain_ref[s, 1])
                moved = tuple(pltpu.roll(value[c], 1 << s, 0) for c in range(2))
                value = cadd(value, cmul(step, moved))
            x.append(value)
        total_t = [None] * active
        for turn in range(2):
            inner = []
            for j in range(active):
                acc = (nil, nil)
                for i in range(len(basis_u[j])):
                    acc = cadd(acc, conj_mul(basis_u[j][i], x[i]))
                inner.append(tuple(jnp.sum(acc[c], axis=0, keepdims=True) for c in range(2)))
            for j in range(active):
                for i in range(len(basis_u[j])):
                    x[i] = csub(x[i], cmul(inner[j], basis_u[j][i]))
                total_t[j] = inner[j] if turn == 0 else cadd(total_t[j], inner[j])
        square = nil
        for value in x:
            square = square + (value[0] * value[0] + value[1] * value[1])
        mu = jnp.sqrt(jnp.sum(square, axis=0, keepdims=True))
        mus.append(jnp.broadcast_to(mu, shape))
        basis_u.append([(value[0] / mu, value[1] / mu) for value in x])
        for j in range(active):
            hess[j, k] = tuple(jnp.broadcast_to(total_t[j][c], shape) for c in range(2))
    small_row = lax.broadcasted_iota(jnp.int32, (names, STEPS), 0)
    small_col = lax.broadcasted_iota(jnp.int32, (names, STEPS), 1)
    for p in range(points):
        for c in range(2):
            value = jnp.zeros((names, STEPS), F32)
            for k in range(STEPS):
                for j in range(k + 2):
                    if j <= k:
                        entry = hess[j, k][c]
                    elif c == 0:
                        entry = mus[k]
                    else:
                        continue
                    here = (small_row == j) & (small_col == k)
                    value = jnp.where(here, entry[0:1, p : p + 1], value)
            hess_ref[p, c] = value
    for copy in copies:
        copy.wait()


def call(body, outs, specs, out_specs, scratch=(), limit=16):
    return pl.pallas_call(
        body,
        out_shape=outs,
        in_specs=specs,
        out_specs=out_specs,
        scratch_shapes=list(scratch),
        compiler_params=pltpu.CompilerParams(vmem_limit_bytes=limit * MIB),
    )


def per_device(
    initial_guess_field,
    medium_label,
    principal_entry_addend,
    linearized_block_weight,
    sample_abscissae,
    singularity_locations,
    basis_normalizers,
    spectral_target,
    quasi_periodic_phase,
):
    points, _, rows, columns = initial_guess_field.shape
    blocks, mats, _ = linearized_block_weight.shape
    tiles = columns // LANES
    planes = 2 * points + 1
    total = rows + 2 * HALO
    count = total // SUB
    names = STEPS + 1
    depth = -(-blocks // SUB) * SUB
    levels = (blocks - 1).bit_length()
    devices = lax.axis_size("gx") * lax.axis_size("gy")
    sds = lambda *shape: jax.ShapeDtypeStruct(shape, F32)

    packed = -(-planes * HALO // SUB) * SUB
    near, far = call(
        pack_rows, [sds(packed, columns)] * 2, [VMEM] * 2, [VMEM] * 2, limit=4
    )(initial_guess_field, medium_label)
    far = lax.ppermute(far, "gx", swap_far("gx"))
    near = lax.ppermute(near, "gx", swap_near("gx"))

    table, trig, chain, size = call(
        params,
        [
            sds(8, mats, SUB, LANES),
            sds(points, 2, 2, SUB, LANES),
            sds(levels, 2, depth, LANES),
            sds(SUB, LANES),
        ],
        [SMEM, VMEM, SMEM, SMEM, SMEM, SMEM, SMEM],
        [VMEM] * 4,
        limit=4,
    )(
        principal_entry_addend,
        linearized_block_weight,
        sample_abscissae,
        singularity_locations,
        basis_normalizers,
        spectral_target,
        quasi_periodic_phase,
    )

    full, near, far = call(
        pack_columns,
        [sds(planes, tiles, total, LANES), sds(total, LANES), sds(total, LANES)],
        [VMEM] * 5,
        [VMEM] * 3,
        limit=8,
    )(initial_guess_field, medium_label, near, far, trig)
    far = lax.ppermute(far, "gy", swap_far("gy"))
    near = lax.ppermute(near, "gy", swap_near("gy"))

    wide = (tiles + 1, count, SUB, LANES)
    out, gram = call(
        solve,
        [sds(STEPS, points, 2, tiles, total, LANES), sds(devices, 1, LANES)],
        [VMEM] * 5,
        [VMEM] * 2,
        [
            pltpu.VMEM((planes, total, LANES), F32),
            pltpu.VMEM((6,) + wide, F32),
            pltpu.VMEM((points, 2) + wide, F32),
            pltpu.VMEM((2, points, 2) + wide, F32),
            pltpu.VMEM((points, 2) + wide, F32),
        ],
        limit=32,
    )(full, near, far, table, trig)

    part = lax.all_to_all(gram, ("gx", "gy"), 0, 0, tiled=True)

    basis, hess = call(
        finish,
        [sds(points, STEPS, 2, rows, columns), sds(points, 2, names, STEPS)],
        [VMEM] * 5,
        [ANY, VMEM],
        [
            pltpu.VMEM((points, STEPS, 2, rows, columns), F32),
            pltpu.SemaphoreType.DMA((points,)),
        ],
        limit=16,
    )(full, out, part, chain, size)
    return basis, hess


def solution(mesh):
    return jax.shard_map(
        per_device,
        mesh=mesh,
        in_specs=(P(None, None, "gx", "gy"), P("gx", "gy"), P(), P(), P(), P(), P(), P(), P()),
        out_specs=(P(None, None, None, "gx", "gy"), P()),
        check_vma=False,
    )
```

```python
import jax
import jax.numpy as jnp
from jax import lax
from jax.experimental import pallas as pl
from jax.experimental.pallas import tpu as pltpu
from jax.sharding import PartitionSpec as P


STEPS = 3
SWEEPS = 4
HALO = STEPS * SWEEPS
LANES = 128
SUB = 8
SLOT = 16
F32 = jnp.float32
VMEM = pl.BlockSpec(memory_space=pltpu.VMEM)
SMEM = pl.BlockSpec(memory_space=pltpu.SMEM)
ANY = pl.BlockSpec(memory_space=pl.ANY)
HBM = pl.BlockSpec(memory_space=pltpu.HBM)
MIB = 1024 * 1024


def even(axis):
    return lax.rem(lax.axis_index(axis), 2) == 0


def swap_near(axis):
    return [(i, i ^ 1) for i in range(lax.axis_size(axis))]


def swap_far(axis):
    n = lax.axis_size(axis)
    return [(i, (i + 1) % n if i % 2 else (i - 1) % n) for i in range(n)]


def cmul(a, b):
    return (a[0] * b[0] - a[1] * b[1], a[0] * b[1] + a[1] * b[0])


def cadd(a, b):
    return (a[0] + b[0], a[1] + b[1])


def csub(a, b):
    return (a[0] - b[0], a[1] - b[1])


def conj_mul(a, b):
    return (a[0] * b[0] + a[1] * b[1], a[0] * b[1] - a[1] * b[0])


def pack_lanes(sides):
    y_even = even("gy")
    shape = sides[0][0].shape
    lane = lax.broadcasted_iota(jnp.int32, shape, 1)
    near_acc = jnp.zeros(shape, F32)
    far_acc = jnp.zeros(shape, F32)
    for plane, (left, right) in enumerate(sides):
        base = plane * SLOT
        keep = (lane >= base) & (lane < base + HALO)
        to_left = jnp.int32(base)
        to_right = jnp.int32((base + HALO) % LANES)
        near = pltpu.roll(jnp.where(y_even, right, left), jnp.where(y_even, to_right, to_left), 1)
        far = pltpu.roll(jnp.where(y_even, left, right), jnp.where(y_even, to_left, to_right), 1)
        near_acc = jnp.where(keep, near, near_acc)
        far_acc = jnp.where(keep, far, far_acc)
    return near_acc, far_acc


def pack_corners(near_x, far_x, near_c, far_c, side_ref):
    planes = side_ref.shape[0]
    columns = near_x.shape[1]
    x_even = even("gx")
    for plane in range(planes):
        span = slice(plane * HALO, (plane + 1) * HALO)
        for side, lanes in enumerate((slice(0, LANES), slice(columns - LANES, columns))):
            near = near_x[span, lanes]
            far = far_x[span, lanes]
            side_ref[plane, side, 0:HALO, :] = jnp.where(x_even, near, far)
            side_ref[plane, side, HALO : 2 * HALO, :] = jnp.where(x_even, far, near)
    near_c[...], far_c[...] = pack_lanes([(side_ref[p, 0], side_ref[p, 1]) for p in range(planes)])


def pack(z_hbm, m_hbm, a_hbm, w_hbm, node_hbm, pole_hbm, scale_hbm, target_hbm, phase_hbm,
         full_ref, near_x, far_x, near_y, far_y,
         a_ref, w_ref, node_ref, pole_ref, scale_ref, target_ref, phase_ref, label_ref, sem):
    points, _, rows, columns = z_hbm.shape
    tiles = columns // LANES
    planes = 2 * points + 1
    pairs = []
    for t in range(tiles):
        lanes = pl.ds(t * LANES, LANES)
        for plane in range(2 * points):
            src = z_hbm.at[plane // 2, plane % 2, :, lanes]
            pairs.append((src, full_ref.at[plane, t, pl.ds(0, rows), :]))
        pairs.append((m_hbm.at[:, lanes], label_ref.at[t]))
    pairs += [(a_hbm, a_ref), (w_hbm, w_ref), (node_hbm, node_ref), (pole_hbm, pole_ref)]
    pairs += [(scale_hbm, scale_ref), (target_hbm, target_ref), (phase_hbm, phase_ref)]
    copies = [pltpu.make_async_copy(src, dst, sem.at[n]) for n, (src, dst) in enumerate(pairs)]
    for copy in copies:
        copy.start()
    for copy in copies:
        copy.wait()
    for t in range(tiles):
        full_ref[planes - 1, t, 0:rows, :] = label_ref[t].astype(F32)
    x_even = even("gx")
    sides = [(full_ref[p, 0, 0:rows, :], full_ref[p, tiles - 1, 0:rows, :]) for p in range(planes)]
    near_acc, far_acc = pack_lanes(sides)
    near_y[...] = near_acc
    far_y[...] = far_acc
    for plane in range(planes):
        span = slice(plane * HALO, (plane + 1) * HALO)
        for t in range(tiles):
            lanes = slice(t * LANES, (t + 1) * LANES)
            top = full_ref[plane, t, 0:HALO, :]
            bottom = full_ref[plane, t, rows - HALO : rows, :]
            near_x[span, lanes] = jnp.where(x_even, bottom, top)
            far_x[span, lanes] = jnp.where(x_even, top, bottom)


def params(a_ref, w_ref, node_ref, pole_ref, scale_ref, target_ref, phase_ref,
           table_ref, trig_ref, chain_ref, size_ref):
    shape = (SUB, LANES)

    def full(value):
        return jnp.broadcast_to(value, shape)

    mats = a_ref.shape[1]
    totals = node_ref.shape[1]
    target = (target_ref[:, 0:1], target_ref[:, 1:2])
    gap = csub(target, (node_ref[0:1, :], node_ref[1:2, :]))
    pole = (pole_ref[0:1, :], pole_ref[1:2, :])
    pole_size = pole[0] * pole[0] + pole[1] * pole[1]
    quotient = conj_mul(pole, target)
    quotient = (quotient[0] / pole_size, quotient[1] / pole_size)
    scale = scale_ref[...]
    lower = (scale * (1.0 - quotient[0]), -scale * quotient[1])
    lower_size = lower[0] * lower[0] + lower[1] * lower[1]
    factor = conj_mul(lower, gap)
    factor = (factor[0] / lower_size, factor[1] / lower_size)
    steps = [tuple(full(factor[c][:, j : j + 1]) for c in range(2)) for j in range(totals)]
    zero = jnp.zeros(shape, F32)
    lane = lax.broadcasted_iota(jnp.int32, shape, 1)
    power = (jnp.ones(shape, F32), zero)
    size = jnp.ones(shape, F32)
    powers = [jnp.where(lane == 0, power[0], zero), zero]
    for b in range(1, totals + 1):
        power = cmul(power, steps[b - 1])
        size = size + (power[0] * power[0] + power[1] * power[1])
        for c in range(2):
            powers[c] = jnp.where(lane == b, power[c], powers[c])
    gamma = jnp.sqrt(size)
    size_ref[...] = gamma
    blocks = totals + 1
    line = tuple((powers[c] / gamma)[0:1, :blocks] for c in range(2))
    order = lax.broadcasted_iota(jnp.int32, (1, blocks), 1).astype(F32)
    for m in range(mats):
        center = 4.0 + full(a_ref[0:1, m : m + 1])
        side = full(a_ref[1:2, m : m + 1])
        inverse_size = center * center + side * side
        inverse = (center / inverse_size, -side / inverse_size)
        w = (w_ref[m, 0:1, :], w_ref[m, 1:2, :])
        first = (full(w[0][:, 0:1]), full(w[1][:, 0:1]))
        product = cmul(w, line)
        a_weight = tuple(full(jnp.sum(p, axis=1, keepdims=True)) for p in product)
        b_weight = tuple(full(jnp.sum(p * order, axis=1, keepdims=True)) for p in product)
        b_weight = (b_weight[0] / gamma, b_weight[1] / gamma)
        entries = (inverse, cmul(inverse, first), cmul(inverse, a_weight), cmul(inverse, b_weight))
        for e, (re, im) in enumerate(entries):
            table_ref[2 * e, m] = re
            table_ref[2 * e + 1, m] = im
    for k in range(phase_ref.shape[0]):
        for axis in range(2):
            angle = full(phase_ref[k : k + 1, axis : axis + 1])
            trig_ref[k, axis, 0] = jnp.cos(angle)
            trig_ref[k, axis, 1] = jnp.sin(angle)
    depth = chain_ref.shape[2]
    row = lax.broadcasted_iota(jnp.int32, shape, 0)
    tiles = [[], []]
    for c in range(2):
        for t in range(depth // SUB):
            value = zero
            for r in range(SUB):
                b = t * SUB + r
                if 1 <= b <= totals:
                    value = jnp.where(row == r, steps[b - 1][c], value)
            tiles[c].append(value)
    step = tuple(jnp.concatenate(tile, 0) for tile in tiles)
    for s in range(chain_ref.shape[0]):
        chain_ref[s, 0] = step[0]
        chain_ref[s, 1] = step[1]
        moved = (pltpu.roll(step[0], 1 << s, 0), pltpu.roll(step[1], 1 << s, 0))
        step = cmul(step, moved)


def solve(own_ref, near_x, far_x, near_y, far_y, near_c, far_c,
          table_ref, trig_ref, out_ref, gram_ref,
          full_ref, edge_ref, halo_ref, cell_ref, b_ref, x_ref, keep_ref):
    planes, tiles, total, _ = own_ref.shape
    points = planes // 2
    rows = total - 2 * HALO
    mats = table_ref.shape[1]
    count = total // SUB
    x_even = even("gx")
    y_even = even("gy")

    for plane in range(planes):
        span = slice(plane * HALO, (plane + 1) * HALO)
        for t in range(tiles):
            lanes = slice(t * LANES, (t + 1) * LANES)
            near = near_x[span, lanes]
            far = far_x[span, lanes]
            full_ref[plane, t, 0:rows, :] = own_ref[plane, t, 0:rows, :]
            full_ref[plane, t, rows : rows + HALO, :] = jnp.where(x_even, near, far)
            full_ref[plane, t, rows + HALO : total, :] = jnp.where(x_even, far, near)
    for side in range(2):
        keep = y_even if side == 0 else jnp.logical_not(y_even)
        edge_ref[side, 0:rows, :] = jnp.where(keep, near_y[...], far_y[...])
        edge_ref[side, rows:total, :] = jnp.where(keep, near_c[...], far_c[...])

    lane = lax.broadcasted_iota(jnp.int32, (total, LANES), 1)
    is_right = lane < HALO
    is_left = lane >= LANES - HALO
    right_src = edge_ref[0]
    left_src = edge_ref[1]
    for plane in range(planes):
        right = pltpu.roll(right_src, (LANES - plane * SLOT) % LANES, 1)
        left = pltpu.roll(left_src, (LANES - HALO - plane * SLOT) % LANES, 1)
        halo_ref[plane] = jnp.where(is_right, right, jnp.where(is_left, left, 0.0))

    def ends(axis):
        first = (lax.axis_index(axis) == 0).astype(F32)
        last = (lax.axis_index(axis) == lax.axis_size(axis) - 1).astype(F32)
        return first, last

    first, last = ends("gx")
    low = lax.broadcasted_iota(jnp.int32, (2 * HALO, LANES), 0) < HALO
    x_edge = jnp.where(low, last, first) > 0.5
    first, last = ends("gy")
    y_edge = jnp.where(is_right, last, jnp.where(is_left, first, 0.0)) > 0.5
    for k in range(points):
        sine = trig_ref[k, 0, 1][0:1, :]
        co = jnp.where(x_edge, trig_ref[k, 0, 0][0:1, :], 1.0)
        si = jnp.where(x_edge, jnp.where(low, sine, -sine), 0.0)
        for t in range(tiles + 1):
            if t < tiles:
                parts = (full_ref.at[2 * k, t], full_ref.at[2 * k + 1, t])
            else:
                parts = (halo_ref.at[2 * k], halo_ref.at[2 * k + 1])
            turned = cmul((parts[0][rows:total, :], parts[1][rows:total, :]), (co, si))
            parts[0][rows:total, :] = turned[0]
            parts[1][rows:total, :] = turned[1]
        sine = trig_ref[k, 1, 1][0:1, :]
        co = jnp.where(y_edge, trig_ref[k, 1, 0][0:1, :], 1.0)
        si = jnp.where(y_edge, jnp.where(is_right, sine, -sine), 0.0)
        turned = cmul((halo_ref[2 * k], halo_ref[2 * k + 1]), (co, si))
        halo_ref[2 * k] = turned[0]
        halo_ref[2 * k + 1] = turned[1]

    def rows_of(plane, t, v):
        span = pl.ds(v, SUB, stride=count)
        if t < tiles:
            return full_ref[plane, t, span, :]
        return halo_ref[plane, span, :]

    for t in range(tiles + 1):
        for v in range(count):
            label = rows_of(planes - 1, t, v)
            picks = [label == float(m) for m in range(1, mats)]

            def pick(e):
                value = table_ref[e, 0]
                for m in range(1, mats):
                    value = jnp.where(picks[m - 1], table_ref[e, m], value)
                return value

            for e in (0, 1):
                cell_ref[e, t, v] = pick(e)
            for e in (4, 5, 6, 7):
                cell_ref[e - 2, t, v] = pick(e)
            weight = (pick(2), pick(3))
            for k in range(points):
                z = (rows_of(2 * k, t, v), rows_of(2 * k + 1, t, v))
                for c, value in enumerate(cmul(weight, z)):
                    b_ref[k, c, t, v] = value
                    x_ref[0, k, c, t, v] = value

    lane8 = lax.broadcasted_iota(jnp.int32, (SUB, LANES), 1)
    at_first = lane8 == 0
    at_last = lane8 == LANES - 1

    def sweep(i, carry):
        src = lax.rem(i, 2)
        dst = 1 - src
        for k in range(points):
            for v in range(count):
                sides = []
                for c in range(2):
                    mine = [x_ref[src, k, c, t, v] for t in range(tiles + 1)]
                    ahead = [pltpu.roll(value, 1, 1) for value in mine]
                    behind = [pltpu.roll(value, LANES - 1, 1) for value in mine]
                    side = []
                    for t in range(tiles + 1):
                        one = jnp.where(at_first, ahead[t - 1], ahead[t])
                        two = jnp.where(at_last, behind[(t + 1) % (tiles + 1)], behind[t])
                        side.append(one + two)
                    sides.append(side)
                for t in range(tiles + 1):
                    n = []
                    for c in range(2):
                        if v > 0:
                            up = x_ref[src, k, c, t, v - 1]
                        else:
                            up = pltpu.roll(x_ref[src, k, c, t, count - 1], 1, 0)
                        if v < count - 1:
                            down = x_ref[src, k, c, t, v + 1]
                        else:
                            down = pltpu.roll(x_ref[src, k, c, t, 0], SUB - 1, 0)
                        n.append(sides[c][t] + (up + down))
                    inverse = (cell_ref[0, t, v], cell_ref[1, t, v])
                    n = cmul(inverse, n)
                    for c in range(2):
                        x_ref[dst, k, c, t, v] = b_ref[k, c, t, v] + n[c]
        return carry

    for s in range(STEPS):
        lax.fori_loop(0, SWEEPS, sweep, 0)
        final = SWEEPS % 2
        for k in range(points):
            for t in range(tiles + 1):
                for v in range(count):
                    y = (x_ref[final, k, 0, t, v], x_ref[final, k, 1, t, v])
                    if t < tiles:
                        for c in range(2):
                            out_ref[s, k, c, t, pl.ds(v, SUB, stride=count), :] = y[c]
                    if s < STEPS - 1:
                        b = cmul((cell_ref[2, t, v], cell_ref[3, t, v]), y)
                        if s == 0:
                            keep = cmul((cell_ref[4, t, v], cell_ref[5, t, v]), y)
                            for c in range(2):
                                keep_ref[k, c, t, v] = keep[c]
                        else:
                            b = cadd(b, (keep_ref[k, 0, t, v], keep_ref[k, 1, t, v]))
                        for c in range(2):
                            b_ref[k, c, t, v] = b[c]
                            x_ref[0, k, c, t, v] = b[c]

    names = STEPS + 1
    zero = jnp.zeros((SUB, LANES), F32)
    line = jnp.zeros((1, LANES), F32)
    lane1 = lax.broadcasted_iota(jnp.int32, (1, LANES), 1)
    entries = [(i, j) for i in range(names) for j in range(i, names)]
    for k in range(points):

        def gather(r, accs):
            accs = list(accs)
            span = pl.ds(pl.multiple_of(r * SUB, SUB), SUB)
            for t in range(tiles):
                fields = [(full_ref[2 * k, t, span, :], full_ref[2 * k + 1, t, span, :])]
                for s in range(STEPS):
                    fields.append((out_ref[s, k, 0, t, span, :], out_ref[s, k, 1, t, span, :]))
                at = 0
                for i, j in entries:
                    if i == j:
                        a = fields[i]
                        accs[at] = accs[at] + (a[0] * a[0] + a[1] * a[1])
                        at += 1
                    else:
                        product = conj_mul(fields[i], fields[j])
                        accs[at] = accs[at] + product[0]
                        accs[at + 1] = accs[at + 1] + product[1]
                        at += 2
            return tuple(accs)

        accs = lax.fori_loop(0, rows // SUB, gather, (zero,) * (names * names))
        for e, acc in enumerate(accs):
            value = jnp.sum(jnp.sum(acc, axis=0, keepdims=True), axis=1, keepdims=True)
            line = jnp.where(lane1 == k * names * names + e, value, line)
    gram_ref[...] = jnp.broadcast_to(line[None], gram_ref.shape)


def finish(full_ref, out_ref, part_ref, chain_ref, size_ref, basis_ref, hess_ref, done_ref, sem):
    planes, tiles, total, _ = full_ref.shape
    points = planes // 2
    rows = total - 2 * HALO
    names = STEPS + 1
    shape = (SUB, LANES)
    line = jnp.sum(part_ref[:, 0, :], axis=0, keepdims=True)
    uppers = []
    inverses = []
    copies = []
    for k in range(points):
        base = k * names * names
        gram = {}
        at = base
        for i in range(names):
            for j in range(i, names):
                width = 1 if i == j else 2
                gram[i, j] = tuple(
                    jnp.broadcast_to(line[:, at + c : at + c + 1], shape) for c in range(width)
                )
                at += width
        upper = {}
        inv = []
        for i in range(names):
            pivot = gram[i, i][0]
            for l in range(i):
                pivot = pivot - (upper[l, i][0] * upper[l, i][0] + upper[l, i][1] * upper[l, i][1])
            root = jnp.sqrt(pivot)
            upper[i, i] = root
            inv.append(1.0 / root)
            for j in range(i + 1, names):
                value = gram[i, j]
                for l in range(i):
                    value = csub(value, conj_mul(upper[l, i], upper[l, j]))
                upper[i, j] = (value[0] * inv[i], value[1] * inv[i])
        uppers.append(upper)
        inverses.append(inv)

        def combine(r, carry):
            span = pl.ds(pl.multiple_of(r * SUB, SUB), SUB)
            for t in range(tiles):
                lanes = slice(t * LANES, (t + 1) * LANES)
                fields = [(full_ref[2 * k, t, span, :], full_ref[2 * k + 1, t, span, :])]
                for s in range(STEPS):
                    fields.append((out_ref[s, k, 0, t, span, :], out_ref[s, k, 1, t, span, :]))
                found = []
                for i in range(names):
                    value = fields[i]
                    for l in range(i):
                        value = csub(value, cmul(upper[l, i], found[l]))
                    value = (value[0] * inv[i], value[1] * inv[i])
                    found.append(value)
                    if i > 0:
                        done_ref[k, i - 1, 0, span, lanes] = value[0]
                        done_ref[k, i - 1, 1, span, lanes] = value[1]
            return carry

        lax.fori_loop(0, rows // SUB, combine, 0)
        copy = pltpu.make_async_copy(done_ref.at[k], basis_ref.at[k], sem.at[k])
        copy.start()
        copies.append(copy)

    lane = lax.broadcasted_iota(jnp.int32, shape, 1)

    def mixed(pick):
        value = pick(0)
        for k in range(1, points):
            value = jnp.where(lane == k, pick(k), value)
        return value

    gamma = size_ref[...]
    inv0 = mixed(lambda k: inverses[k][0])
    column = []
    for j in range(1, names):
        entry = []
        for i in range(j):
            entry.append(tuple(mixed(lambda k: uppers[k][i, j][c]) * inv0 for c in range(2)))
        entry.append((mixed(lambda k: uppers[k][j, j]) * inv0, jnp.zeros(shape, F32)))
        column.append(entry)

    depth = chain_ref.shape[2]
    row = lax.broadcasted_iota(jnp.int32, (depth, LANES), 0)
    tall = lambda value: jnp.broadcast_to(value[0:1], (depth, LANES))
    nil = jnp.zeros((depth, LANES), F32)
    at_top = row == 0
    basis_u = [[(jnp.where(at_top, 1.0, 0.0), nil)]]
    hess = {}
    coords = []
    mus = []
    for k in range(STEPS):
        active = k + 1
        if k == 0:
            found = column[0]
        elif k == 1:
            found = []
            for i in range(3):
                value = (column[1][i][0] * gamma, column[1][i][1] * gamma)
                if i < 2:
                    value = csub(value, cmul(hess[0, 0], coords[0][i]))
                found.append((value[0] / mus[0], value[1] / mus[0]))
        else:
            found = []
            scale = gamma / mus[0]
            for i in range(4):
                value = (column[2][i][0] * gamma, column[2][i][1] * gamma)
                if i < 3:
                    value = csub(value, cmul(hess[0, 0], column[1][i]))
                value = (value[0] * scale, value[1] * scale)
                if i < 2:
                    value = csub(value, cmul(hess[0, 1], coords[0][i]))
                if i < 3:
                    value = csub(value, cmul(hess[1, 1], coords[1][i]))
                found.append((value[0] / mus[1], value[1] / mus[1]))
        coords.append(found)
        current = basis_u[k]
        x = []
        for i in range(active + 1):
            old = current[i] if i < len(current) else (nil, nil)
            value = tuple(jnp.where(at_top, tall(found[i][c]), old[c]) for c in range(2))
            for s in range(chain_ref.shape[0]):
                step = (chain_ref[s, 0], chain_ref[s, 1])
                moved = tuple(pltpu.roll(value[c], 1 << s, 0) for c in range(2))
                value = cadd(value, cmul(step, moved))
            x.append(value)
        total_t = [None] * active
        for turn in range(2):
            inner = []
            for j in range(active):
                acc = (nil, nil)
                for i in range(len(basis_u[j])):
                    acc = cadd(acc, conj_mul(basis_u[j][i], x[i]))
                inner.append(tuple(jnp.sum(acc[c], axis=0, keepdims=True) for c in range(2)))
            for j in range(active):
                for i in range(len(basis_u[j])):
                    x[i] = csub(x[i], cmul(inner[j], basis_u[j][i]))
                total_t[j] = inner[j] if turn == 0 else cadd(total_t[j], inner[j])
        square = nil
        for value in x:
            square = square + (value[0] * value[0] + value[1] * value[1])
        mu = jnp.sqrt(jnp.sum(square, axis=0, keepdims=True))
        mus.append(jnp.broadcast_to(mu, shape))
        basis_u.append([(value[0] / mu, value[1] / mu) for value in x])
        for j in range(active):
            hess[j, k] = tuple(jnp.broadcast_to(total_t[j][c], shape) for c in range(2))
    part_row = lax.broadcasted_iota(jnp.int32, (2, names), 0)
    part_lane = lax.broadcasted_iota(jnp.int32, (2, names), 1)
    for p in range(points):
        for k in range(STEPS):
            value = jnp.zeros((2, names), F32)
            for j in range(k + 2):
                parts = hess[j, k] if j <= k else (mus[k],)
                for c, entry in enumerate(parts):
                    here = (part_row == c) & (part_lane == j)
                    value = jnp.where(here, entry[0:1, p : p + 1], value)
            hess_ref[p, k] = value
    for copy in copies:
        copy.wait()


def call(body, outs, specs, out_specs, scratch=(), limit=16):
    return pl.pallas_call(
        body,
        out_shape=outs,
        in_specs=specs,
        out_specs=out_specs,
        scratch_shapes=list(scratch),
        compiler_params=pltpu.CompilerParams(vmem_limit_bytes=limit * MIB),
    )


def per_device(
    initial_guess_field,
    medium_label,
    principal_entry_addend,
    linearized_block_weight,
    sample_abscissae,
    singularity_locations,
    basis_normalizers,
    spectral_target,
    quasi_periodic_phase,
):
    points, _, rows, columns = initial_guess_field.shape
    blocks, mats, _ = linearized_block_weight.shape
    tiles = columns // LANES
    planes = 2 * points + 1
    total = rows + 2 * HALO
    count = total // SUB
    names = STEPS + 1
    depth = -(-blocks // SUB) * SUB
    levels = (blocks - 1).bit_length()
    devices = lax.axis_size("gx") * lax.axis_size("gy")
    sds = lambda *shape: jax.ShapeDtypeStruct(shape, F32)

    packed = -(-planes * HALO // SUB) * SUB
    small = [
        principal_entry_addend.T,
        linearized_block_weight.transpose(1, 2, 0),
        sample_abscissae.T,
        singularity_locations.T,
        basis_normalizers.reshape(1, -1),
        spectral_target.reshape(1, -1),
        quasi_periodic_phase,
    ]
    full, *sends = call(
        pack,
        [sds(planes, tiles, total, LANES)]
        + [sds(packed, columns)] * 2
        + [sds(rows, LANES)] * 2
        + [sds(*value.shape) for value in small],
        [HBM] * 9,
        [VMEM] * 12,
        [
            pltpu.VMEM((tiles, rows, LANES), jnp.int32),
            pltpu.SemaphoreType.DMA((tiles * planes + len(small),)),
        ],
        limit=8,
    )(*[pltpu.with_memory_space_constraint(v, pltpu.HBM) for v in (initial_guess_field, medium_label, *small)])
    near_x, far_x, near_y, far_y, *small = sends

    def send(value, axis, pairs):
        return lax.ppermute(value, axis, pairs(axis))

    far_x = send(far_x, "gx", swap_far)
    near_x = send(near_x, "gx", swap_near)
    far_y = send(far_y, "gy", swap_far)
    near_y = send(near_y, "gy", swap_near)

    table, trig, chain, size = call(
        params,
        [
            sds(8, mats, SUB, LANES),
            sds(points, 2, 2, SUB, LANES),
            sds(levels, 2, depth, LANES),
            sds(SUB, LANES),
        ],
        [VMEM] * 7,
        [VMEM] * 4,
        limit=4,
    )(*small)

    near_c, far_c = call(
        pack_corners,
        [sds(2 * HALO, LANES)] * 2,
        [VMEM] * 2,
        [VMEM] * 2,
        [pltpu.VMEM((planes, 2, 2 * HALO, LANES), F32)],
        limit=4,
    )(near_x, far_x)
    far_c = send(far_c, "gy", swap_far)
    near_c = send(near_c, "gy", swap_near)

    wide = (tiles + 1, count, SUB, LANES)
    out, gram = call(
        solve,
        [sds(STEPS, points, 2, tiles, total, LANES), sds(devices, 1, LANES)],
        [VMEM] * 9,
        [VMEM] * 2,
        [
            pltpu.VMEM((planes, tiles, total, LANES), F32),
            pltpu.VMEM((2, total, LANES), F32),
            pltpu.VMEM((planes, total, LANES), F32),
            pltpu.VMEM((6,) + wide, F32),
            pltpu.VMEM((points, 2) + wide, F32),
            pltpu.VMEM((2, points, 2) + wide, F32),
            pltpu.VMEM((points, 2) + wide, F32),
        ],
        limit=32,
    )(
        full, near_x, far_x, near_y, far_y, near_c, far_c, table, trig
    )

    part = lax.all_to_all(gram, ("gx", "gy"), 0, 0, tiled=True)

    basis, hess = call(
        finish,
        [sds(points, STEPS, 2, rows, columns), sds(points, STEPS, 2, names)],
        [VMEM] * 5,
        [ANY, VMEM],
        [
            pltpu.VMEM((points, STEPS, 2, rows, columns), F32),
            pltpu.SemaphoreType.DMA((points,)),
        ],
        limit=16,
    )(full, out, part, chain, size)
    return basis, hess.transpose(0, 2, 3, 1)


def solution(mesh):
    return jax.shard_map(
        per_device,
        mesh=mesh,
        in_specs=(P(None, None, "gx", "gy"), P("gx", "gy"), P(), P(), P(), P(), P(), P(), P()),
        out_specs=(P(None, None, None, "gx", "gy"), P()),
        check_vma=False,
    )
```

```python
import jax
import jax.numpy as jnp
from jax import lax
from jax.experimental import pallas as pl
from jax.experimental.pallas import tpu as pltpu
from jax.sharding import PartitionSpec as P


STEPS = 3
SWEEPS = 4
HALO = STEPS * SWEEPS
LANES = 128
SUB = 8
SLOT = 16
F32 = jnp.float32
VMEM = pl.BlockSpec(memory_space=pltpu.VMEM)
SMEM = pl.BlockSpec(memory_space=pltpu.SMEM)
ANY = pl.BlockSpec(memory_space=pl.ANY)
HBM = pl.BlockSpec(memory_space=pltpu.HBM)
MIB = 1024 * 1024


def even(axis):
    return lax.rem(lax.axis_index(axis), 2) == 0


def swap_near(axis):
    return [(i, i ^ 1) for i in range(lax.axis_size(axis))]


def swap_far(axis):
    n = lax.axis_size(axis)
    return [(i, (i + 1) % n if i % 2 else (i - 1) % n) for i in range(n)]


def cmul(a, b):
    return (a[0] * b[0] - a[1] * b[1], a[0] * b[1] + a[1] * b[0])


def cadd(a, b):
    return (a[0] + b[0], a[1] + b[1])


def csub(a, b):
    return (a[0] - b[0], a[1] - b[1])


def conj_mul(a, b):
    return (a[0] * b[0] + a[1] * b[1], a[0] * b[1] - a[1] * b[0])


def pack_lanes(sides):
    y_even = even("gy")
    shape = sides[0][0].shape
    lane = lax.broadcasted_iota(jnp.int32, shape, 1)
    near_acc = jnp.zeros(shape, F32)
    far_acc = jnp.zeros(shape, F32)
    for plane, (left, right) in enumerate(sides):
        base = plane * SLOT
        keep = (lane >= base) & (lane < base + HALO)
        to_left = jnp.int32(base)
        to_right = jnp.int32((base + HALO) % LANES)
        near = pltpu.roll(jnp.where(y_even, right, left), jnp.where(y_even, to_right, to_left), 1)
        far = pltpu.roll(jnp.where(y_even, left, right), jnp.where(y_even, to_left, to_right), 1)
        near_acc = jnp.where(keep, near, near_acc)
        far_acc = jnp.where(keep, far, far_acc)
    return near_acc, far_acc


def pack_corners(near_x, far_x, near_c, far_c, side_ref):
    planes = side_ref.shape[0]
    columns = near_x.shape[1]
    x_even = even("gx")
    for plane in range(planes):
        span = slice(plane * HALO, (plane + 1) * HALO)
        for side, lanes in enumerate((slice(0, LANES), slice(columns - LANES, columns))):
            near = near_x[span, lanes]
            far = far_x[span, lanes]
            side_ref[plane, side, 0:HALO, :] = jnp.where(x_even, near, far)
            side_ref[plane, side, HALO : 2 * HALO, :] = jnp.where(x_even, far, near)
    near_c[...], far_c[...] = pack_lanes([(side_ref[p, 0], side_ref[p, 1]) for p in range(planes)])


def pack(z_hbm, m_hbm, a_hbm, w_hbm, node_hbm, pole_hbm, scale_hbm, target_hbm, phase_hbm,
         full_ref, near_x, far_x, near_y, far_y,
         a_ref, w_ref, node_ref, pole_ref, scale_ref, target_ref, phase_ref, label_ref, sem):
    points, _, rows, columns = z_hbm.shape
    tiles = columns // LANES
    planes = 2 * points + 1
    pairs = []
    for t in range(tiles):
        lanes = pl.ds(t * LANES, LANES)
        for plane in range(2 * points):
            src = z_hbm.at[plane // 2, plane % 2, :, lanes]
            pairs.append((src, full_ref.at[plane, t, pl.ds(0, rows), :]))
        pairs.append((m_hbm.at[:, lanes], label_ref.at[t]))
    pairs += [(a_hbm, a_ref), (w_hbm, w_ref), (node_hbm, node_ref), (pole_hbm, pole_ref)]
    pairs += [(scale_hbm, scale_ref), (target_hbm, target_ref), (phase_hbm, phase_ref)]
    copies = [pltpu.make_async_copy(src, dst, sem.at[n]) for n, (src, dst) in enumerate(pairs)]
    for copy in copies:
        copy.start()
    for copy in copies:
        copy.wait()
    for t in range(tiles):
        full_ref[planes - 1, t, 0:rows, :] = label_ref[t].astype(F32)
    x_even = even("gx")
    sides = [(full_ref[p, 0, 0:rows, :], full_ref[p, tiles - 1, 0:rows, :]) for p in range(planes)]
    near_acc, far_acc = pack_lanes(sides)
    near_y[...] = near_acc
    far_y[...] = far_acc
    for plane in range(planes):
        span = slice(plane * HALO, (plane + 1) * HALO)
        for t in range(tiles):
            lanes = slice(t * LANES, (t + 1) * LANES)
            top = full_ref[plane, t, 0:HALO, :]
            bottom = full_ref[plane, t, rows - HALO : rows, :]
            near_x[span, lanes] = jnp.where(x_even, bottom, top)
            far_x[span, lanes] = jnp.where(x_even, top, bottom)


def params(a_ref, w_ref, node_ref, pole_ref, scale_ref, target_ref, phase_ref,
           table_ref, trig_ref, chain_ref, size_ref):
    shape = (SUB, LANES)

    def full(value):
        return jnp.broadcast_to(value, shape)

    mats = a_ref.shape[1]
    totals = node_ref.shape[1]
    target = (target_ref[:, 0:1], target_ref[:, 1:2])
    gap = csub(target, (node_ref[0:1, :], node_ref[1:2, :]))
    pole = (pole_ref[0:1, :], pole_ref[1:2, :])
    pole_size = pole[0] * pole[0] + pole[1] * pole[1]
    quotient = conj_mul(pole, target)
    quotient = (quotient[0] / pole_size, quotient[1] / pole_size)
    scale = scale_ref[...]
    lower = (scale * (1.0 - quotient[0]), -scale * quotient[1])
    lower_size = lower[0] * lower[0] + lower[1] * lower[1]
    factor = conj_mul(lower, gap)
    factor = (factor[0] / lower_size, factor[1] / lower_size)
    steps = [tuple(full(factor[c][:, j : j + 1]) for c in range(2)) for j in range(totals)]
    zero = jnp.zeros(shape, F32)
    lane = lax.broadcasted_iota(jnp.int32, shape, 1)
    power = (jnp.ones(shape, F32), zero)
    size = jnp.ones(shape, F32)
    powers = [jnp.where(lane == 0, power[0], zero), zero]
    for b in range(1, totals + 1):
        power = cmul(power, steps[b - 1])
        size = size + (power[0] * power[0] + power[1] * power[1])
        for c in range(2):
            powers[c] = jnp.where(lane == b, power[c], powers[c])
    gamma = jnp.sqrt(size)
    size_ref[...] = gamma
    blocks = totals + 1
    line = tuple((powers[c] / gamma)[0:1, :blocks] for c in range(2))
    order = lax.broadcasted_iota(jnp.int32, (1, blocks), 1).astype(F32)
    for m in range(mats):
        center = 4.0 + full(a_ref[0:1, m : m + 1])
        side = full(a_ref[1:2, m : m + 1])
        inverse_size = center * center + side * side
        inverse = (center / inverse_size, -side / inverse_size)
        w = (w_ref[m, 0:1, :], w_ref[m, 1:2, :])
        first = (full(w[0][:, 0:1]), full(w[1][:, 0:1]))
        product = cmul(w, line)
        a_weight = tuple(full(jnp.sum(p, axis=1, keepdims=True)) for p in product)
        b_weight = tuple(full(jnp.sum(p * order, axis=1, keepdims=True)) for p in product)
        b_weight = (b_weight[0] / gamma, b_weight[1] / gamma)
        entries = (inverse, cmul(inverse, first), cmul(inverse, a_weight), cmul(inverse, b_weight))
        for e, (re, im) in enumerate(entries):
            table_ref[2 * e, m] = re
            table_ref[2 * e + 1, m] = im
    for k in range(phase_ref.shape[0]):
        for axis in range(2):
            angle = full(phase_ref[k : k + 1, axis : axis + 1])
            trig_ref[k, axis, 0] = jnp.cos(angle)
            trig_ref[k, axis, 1] = jnp.sin(angle)
    depth = chain_ref.shape[2]
    row = lax.broadcasted_iota(jnp.int32, shape, 0)
    tiles = [[], []]
    for c in range(2):
        for t in range(depth // SUB):
            value = zero
            for r in range(SUB):
                b = t * SUB + r
                if 1 <= b <= totals:
                    value = jnp.where(row == r, steps[b - 1][c], value)
            tiles[c].append(value)
    step = tuple(jnp.concatenate(tile, 0) for tile in tiles)
    for s in range(chain_ref.shape[0]):
        chain_ref[s, 0] = step[0]
        chain_ref[s, 1] = step[1]
        moved = (pltpu.roll(step[0], 1 << s, 0), pltpu.roll(step[1], 1 << s, 0))
        step = cmul(step, moved)


def spread_lanes(tiles):
    count = len(tiles)
    shape = tiles[0].shape
    lane = lax.broadcasted_iota(jnp.int32, shape, 1)
    owner = lane // (LANES // count)
    result = []
    for j in range(count):
        index = lax.rem(lane * count + j, LANES)
        value = jnp.take_along_axis(tiles[0], index, axis=1)
        for t in range(1, count):
            value = jnp.where(owner == t, jnp.take_along_axis(tiles[t], index, axis=1), value)
        result.append(value)
    return result


def spread(full_ref, own_ref):
    planes, tiles, rows, _ = own_ref.shape
    for plane in range(planes):
        for r in range(0, rows, SUB):
            values = spread_lanes([full_ref[plane, t, r : r + SUB, :] for t in range(tiles)])
            for j, value in enumerate(values):
                own_ref[plane, j, r : r + SUB, :] = value


def picker(label, table_ref):
    mats = table_ref.shape[1]
    picks = [label == float(m) for m in range(1, mats)]

    def pick(e):
        value = table_ref[e, 0]
        for m in range(1, mats):
            value = jnp.where(picks[m - 1], table_ref[e, m], value)
        return value

    return pick


def ends(axis):
    first = (lax.axis_index(axis) == 0).astype(F32)
    last = (lax.axis_index(axis) == lax.axis_size(axis) - 1).astype(F32)
    return first, last


def row_turns(trig_ref, k):
    first, last = ends("gx")
    low = lax.broadcasted_iota(jnp.int32, (2 * HALO, LANES), 0) < HALO
    edge = jnp.where(low, last, first) > 0.5
    sine = trig_ref[k, 0, 1][0:1, :]
    co = jnp.where(edge, trig_ref[k, 0, 0][0:1, :], 1.0)
    return co, jnp.where(edge, jnp.where(low, sine, -sine), 0.0)


def stage(own_ref, near_x, far_x, table_ref, trig_ref, cell_ref, b_ref, raw_ref, work_ref):
    planes, tiles, rows, _ = own_ref.shape
    points = planes // 2
    total = rows + 2 * HALO
    count = total // SUB
    x_even = even("gx")
    for plane in range(planes):
        span = slice(plane * HALO, (plane + 1) * HALO)
        for t in range(tiles):
            lanes = slice(t * LANES, (t + 1) * LANES)
            near = near_x[span, lanes]
            far = far_x[span, lanes]
            raw_ref[plane, t, 0:HALO, :] = jnp.where(x_even, near, far)
            raw_ref[plane, t, HALO : 2 * HALO, :] = jnp.where(x_even, far, near)
            work_ref[plane, t, 0:rows, :] = own_ref[plane, t]
    for k in range(points):
        turn = row_turns(trig_ref, k)
        for t in range(tiles):
            turned = cmul((raw_ref[2 * k, t], raw_ref[2 * k + 1, t]), turn)
            raw_ref[2 * k, t] = turned[0]
            raw_ref[2 * k + 1, t] = turned[1]
    for plane in range(planes):
        for r in range(0, 2 * HALO, SUB):
            values = spread_lanes([raw_ref[plane, t, r : r + SUB, :] for t in range(tiles)])
            for j, value in enumerate(values):
                work_ref[plane, j, rows + r : rows + r + SUB, :] = value
    for j in range(tiles):
        for v in range(count):
            span = pl.ds(v, SUB, stride=count)
            pick = picker(work_ref[planes - 1, j, span, :], table_ref)
            for n, e in enumerate((0, 1, 4, 5, 6, 7)):
                cell_ref[n, j, v] = pick(e)
            weight = (pick(2), pick(3))
            for k in range(points):
                z = (work_ref[2 * k, j, span, :], work_ref[2 * k + 1, j, span, :])
                for c, value in enumerate(cmul(weight, z)):
                    b_ref[k, c, j, v] = value


def solve(own_ref, near_y, far_y, near_c, far_c, table_ref, trig_ref, cell_own, b_own,
          out_ref, gram_ref, edge_ref, halo_ref, cell_halo, b_ref, x_ref, w_ref, keep_ref):
    planes, tiles, rows, _ = own_ref.shape
    points = planes // 2
    total = rows + 2 * HALO
    count = total // SUB
    y_even = even("gy")
    for side in range(2):
        keep = y_even if side == 0 else jnp.logical_not(y_even)
        edge_ref[side, 0:rows, :] = jnp.where(keep, near_y[...], far_y[...])
        edge_ref[side, rows:total, :] = jnp.where(keep, near_c[...], far_c[...])
    lane = lax.broadcasted_iota(jnp.int32, (total, LANES), 1)
    is_right = lane < HALO
    is_left = lane >= LANES - HALO
    right_src = edge_ref[0]
    left_src = edge_ref[1]
    for plane in range(planes):
        right = pltpu.roll(right_src, (LANES - plane * SLOT) % LANES, 1)
        left = pltpu.roll(left_src, (LANES - HALO - plane * SLOT) % LANES, 1)
        halo_ref[plane] = jnp.where(is_right, right, jnp.where(is_left, left, 0.0))
    first, last = ends("gy")
    y_edge = jnp.where(is_right, last, jnp.where(is_left, first, 0.0)) > 0.5
    for k in range(points):
        turned = cmul(
            (halo_ref[2 * k, rows:total, :], halo_ref[2 * k + 1, rows:total, :]),
            row_turns(trig_ref, k),
        )
        halo_ref[2 * k, rows:total, :] = turned[0]
        halo_ref[2 * k + 1, rows:total, :] = turned[1]
        sine = trig_ref[k, 1, 1][0:1, :]
        co = jnp.where(y_edge, trig_ref[k, 1, 0][0:1, :], 1.0)
        si = jnp.where(y_edge, jnp.where(is_right, sine, -sine), 0.0)
        turned = cmul((halo_ref[2 * k], halo_ref[2 * k + 1]), (co, si))
        halo_ref[2 * k] = turned[0]
        halo_ref[2 * k + 1] = turned[1]
    for v in range(count):
        span = pl.ds(v, SUB, stride=count)
        pick = picker(halo_ref[planes - 1, span, :], table_ref)
        for n, e in enumerate((0, 1, 4, 5, 6, 7)):
            cell_halo[n, v] = pick(e)
        weight = (pick(2), pick(3))
        for k in range(points):
            z = (halo_ref[2 * k, span, :], halo_ref[2 * k + 1, span, :])
            for c, value in enumerate(cmul(weight, z)):
                b_ref[k, c, tiles, v] = value
                x_ref[k, c, tiles, v] = value
                for t in range(tiles):
                    own = b_own[k, c, t, v]
                    b_ref[k, c, t, v] = own
                    x_ref[k, c, t, v] = own

    def cell(e, t, v):
        return cell_own[e, t, v] if t < tiles else cell_halo[e, v]

    lane8 = lax.broadcasted_iota(jnp.int32, (SUB, LANES), 1)
    at_first = lane8 == 0
    at_last = lane8 == LANES - 1

    def sweep(src_ref, dst_ref):
        for k in range(points):
            for v in range(count):
                sides = []
                for c in range(2):
                    x = [src_ref[k, c, t, v] for t in range(tiles + 1)]
                    last_on = pltpu.roll(x[tiles - 1], 1, 1)
                    halo_on = pltpu.roll(x[tiles], 1, 1)
                    first_back = pltpu.roll(x[0], LANES - 1, 1)
                    halo_back = pltpu.roll(x[tiles], LANES - 1, 1)
                    left = [jnp.where(at_first, halo_on, last_on)] + x[: tiles - 1]
                    right = x[1:tiles] + [jnp.where(at_last, halo_back, first_back)]
                    side = [a + b for a, b in zip(left, right)]
                    one = jnp.where(at_first, last_on, halo_on)
                    two = jnp.where(at_last, first_back, halo_back)
                    sides.append(side + [one + two])
                for t in range(tiles + 1):
                    n = []
                    for c in range(2):
                        if v > 0:
                            up = src_ref[k, c, t, v - 1]
                        else:
                            up = pltpu.roll(src_ref[k, c, t, count - 1], 1, 0)
                        if v < count - 1:
                            down = src_ref[k, c, t, v + 1]
                        else:
                            down = pltpu.roll(src_ref[k, c, t, 0], SUB - 1, 0)
                        n.append(sides[c][t] + (up + down))
                    n = cmul((cell(0, t, v), cell(1, t, v)), n)
                    for c in range(2):
                        dst_ref[k, c, t, v] = b_ref[k, c, t, v] + n[c]

    def pair(i, carry):
        sweep(x_ref, w_ref)
        sweep(w_ref, x_ref)
        return carry

    for s in range(STEPS):
        lax.fori_loop(0, SWEEPS // 2, pair, 0)
        for k in range(points):
            for t in range(tiles + 1):
                for v in range(count):
                    y = (x_ref[k, 0, t, v], x_ref[k, 1, t, v])
                    if t < tiles:
                        for c in range(2):
                            out_ref[s, k, c, t, pl.ds(v, SUB, stride=count), :] = y[c]
                    if s < STEPS - 1:
                        b = cmul((cell(2, t, v), cell(3, t, v)), y)
                        if s == 0:
                            keep = cmul((cell(4, t, v), cell(5, t, v)), y)
                            for c in range(2):
                                keep_ref[k, c, t, v] = keep[c]
                        else:
                            b = cadd(b, (keep_ref[k, 0, t, v], keep_ref[k, 1, t, v]))
                        for c in range(2):
                            b_ref[k, c, t, v] = b[c]
                            x_ref[k, c, t, v] = b[c]

    names = STEPS + 1
    zero = jnp.zeros((SUB, LANES), F32)
    line = jnp.zeros((1, LANES), F32)
    lane1 = lax.broadcasted_iota(jnp.int32, (1, LANES), 1)
    entries = [(i, j) for i in range(names) for j in range(i, names)]
    for k in range(points):

        def gather(r, accs):
            accs = list(accs)
            span = pl.ds(pl.multiple_of(r * SUB, SUB), SUB)
            for t in range(tiles):
                fields = [(own_ref[2 * k, t, span, :], own_ref[2 * k + 1, t, span, :])]
                for s in range(STEPS):
                    fields.append((out_ref[s, k, 0, t, span, :], out_ref[s, k, 1, t, span, :]))
                at = 0
                for i, j in entries:
                    if i == j:
                        a = fields[i]
                        accs[at] = accs[at] + (a[0] * a[0] + a[1] * a[1])
                        at += 1
                    else:
                        product = conj_mul(fields[i], fields[j])
                        accs[at] = accs[at] + product[0]
                        accs[at + 1] = accs[at + 1] + product[1]
                        at += 2
            return tuple(accs)

        accs = lax.fori_loop(0, rows // SUB, gather, (zero,) * (names * names))
        for e, acc in enumerate(accs):
            value = jnp.sum(jnp.sum(acc, axis=0, keepdims=True), axis=1, keepdims=True)
            line = jnp.where(lane1 == k * names * names + e, value, line)
    gram_ref[...] = jnp.broadcast_to(line[None], gram_ref.shape)


def finish(own_ref, out_ref, part_ref, chain_ref, size_ref, basis_ref, hess_ref,
           found_ref, turn_ref, done_ref, sem):
    planes, tiles, rows, _ = own_ref.shape
    points = planes // 2
    names = STEPS + 1
    shape = (SUB, LANES)
    line = jnp.sum(part_ref[:, 0, :], axis=0, keepdims=True)
    uppers = []
    inverses = []
    copies = []
    for k in range(points):
        base = k * names * names
        gram = {}
        at = base
        for i in range(names):
            for j in range(i, names):
                width = 1 if i == j else 2
                gram[i, j] = tuple(
                    jnp.broadcast_to(line[:, at + c : at + c + 1], shape) for c in range(width)
                )
                at += width
        upper = {}
        inv = []
        for i in range(names):
            pivot = gram[i, i][0]
            for l in range(i):
                pivot = pivot - (upper[l, i][0] * upper[l, i][0] + upper[l, i][1] * upper[l, i][1])
            root = jnp.sqrt(pivot)
            upper[i, i] = root
            inv.append(1.0 / root)
            for j in range(i + 1, names):
                value = gram[i, j]
                for l in range(i):
                    value = csub(value, conj_mul(upper[l, i], upper[l, j]))
                upper[i, j] = (value[0] * inv[i], value[1] * inv[i])
        uppers.append(upper)
        inverses.append(inv)

        def combine(r, carry):
            span = pl.ds(pl.multiple_of(r * SUB, SUB), SUB)
            for t in range(tiles):
                fields = [(own_ref[2 * k, t, span, :], own_ref[2 * k + 1, t, span, :])]
                for s in range(STEPS):
                    fields.append((out_ref[s, k, 0, t, span, :], out_ref[s, k, 1, t, span, :]))
                found = []
                for i in range(names):
                    value = fields[i]
                    for l in range(i):
                        value = csub(value, cmul(upper[l, i], found[l]))
                    value = (value[0] * inv[i], value[1] * inv[i])
                    found.append(value)
                    if i > 0:
                        for c in range(2):
                            place = pl.ds(pl.multiple_of(c * rows + r * SUB, SUB), SUB)
                            found_ref[i - 1, t, place, :] = value[c]
            return carry

        lax.fori_loop(0, rows // SUB, combine, 0)
        for i in range(STEPS):
            for n in range(0, 2 * rows, LANES):
                for t in range(tiles):
                    turned = found_ref[i, t, n : n + LANES, :].T
                    turn_ref[i, pl.ds(t, LANES, stride=tiles), :] = turned
                for t in range(tiles):
                    lanes = slice(t * LANES, (t + 1) * LANES)
                    done_ref[k, i, n : n + LANES, lanes] = turn_ref[i, lanes, :].T
            copy = pltpu.make_async_copy(done_ref.at[k, i], basis_ref.at[k, i], sem.at[k, i])
            copy.start()
            copies.append(copy)

    lane = lax.broadcasted_iota(jnp.int32, shape, 1)

    def mixed(pick):
        value = pick(0)
        for k in range(1, points):
            value = jnp.where(lane == k, pick(k), value)
        return value

    gamma = size_ref[...]
    inv0 = mixed(lambda k: inverses[k][0])
    column = []
    for j in range(1, names):
        entry = []
        for i in range(j):
            entry.append(tuple(mixed(lambda k: uppers[k][i, j][c]) * inv0 for c in range(2)))
        entry.append((mixed(lambda k: uppers[k][j, j]) * inv0, jnp.zeros(shape, F32)))
        column.append(entry)

    depth = chain_ref.shape[2]
    row = lax.broadcasted_iota(jnp.int32, (depth, LANES), 0)
    tall = lambda value: jnp.broadcast_to(value[0:1], (depth, LANES))
    nil = jnp.zeros((depth, LANES), F32)
    at_top = row == 0
    basis_u = [[(jnp.where(at_top, 1.0, 0.0), nil)]]
    hess = {}
    coords = []
    mus = []
    for k in range(STEPS):
        active = k + 1
        if k == 0:
            found = column[0]
        elif k == 1:
            found = []
            for i in range(3):
                value = (column[1][i][0] * gamma, column[1][i][1] * gamma)
                if i < 2:
                    value = csub(value, cmul(hess[0, 0], coords[0][i]))
                found.append((value[0] / mus[0], value[1] / mus[0]))
        else:
            found = []
            scale = gamma / mus[0]
            for i in range(4):
                value = (column[2][i][0] * gamma, column[2][i][1] * gamma)
                if i < 3:
                    value = csub(value, cmul(hess[0, 0], column[1][i]))
                value = (value[0] * scale, value[1] * scale)
                if i < 2:
                    value = csub(value, cmul(hess[0, 1], coords[0][i]))
                if i < 3:
                    value = csub(value, cmul(hess[1, 1], coords[1][i]))
                found.append((value[0] / mus[1], value[1] / mus[1]))
        coords.append(found)
        current = basis_u[k]
        x = []
        for i in range(active + 1):
            old = current[i] if i < len(current) else (nil, nil)
            value = tuple(jnp.where(at_top, tall(found[i][c]), old[c]) for c in range(2))
            for s in range(chain_ref.shape[0]):
                step = (chain_ref[s, 0], chain_ref[s, 1])
                moved = tuple(pltpu.roll(value[c], 1 << s, 0) for c in range(2))
                value = cadd(value, cmul(step, moved))
            x.append(value)
        total_t = [None] * active
        for turn in range(2):
            inner = []
            for j in range(active):
                acc = (nil, nil)
                for i in range(len(basis_u[j])):
                    acc = cadd(acc, conj_mul(basis_u[j][i], x[i]))
                inner.append(tuple(jnp.sum(acc[c], axis=0, keepdims=True) for c in range(2)))
            for j in range(active):
                for i in range(len(basis_u[j])):
                    x[i] = csub(x[i], cmul(inner[j], basis_u[j][i]))
                total_t[j] = inner[j] if turn == 0 else cadd(total_t[j], inner[j])
        square = nil
        for value in x:
            square = square + (value[0] * value[0] + value[1] * value[1])
        mu = jnp.sqrt(jnp.sum(square, axis=0, keepdims=True))
        mus.append(jnp.broadcast_to(mu, shape))
        basis_u.append([(value[0] / mu, value[1] / mu) for value in x])
        for j in range(active):
            hess[j, k] = tuple(jnp.broadcast_to(total_t[j][c], shape) for c in range(2))
    part_row = lax.broadcasted_iota(jnp.int32, (2, names), 0)
    part_lane = lax.broadcasted_iota(jnp.int32, (2, names), 1)
    for p in range(points):
        for k in range(STEPS):
            value = jnp.zeros((2, names), F32)
            for j in range(k + 2):
                parts = hess[j, k] if j <= k else (mus[k],)
                for c, entry in enumerate(parts):
                    here = (part_row == c) & (part_lane == j)
                    value = jnp.where(here, entry[0:1, p : p + 1], value)
            hess_ref[p, k] = value
    for copy in copies:
        copy.wait()


def call(body, outs, specs, out_specs, scratch=(), limit=16):
    return pl.pallas_call(
        body,
        out_shape=outs,
        in_specs=specs,
        out_specs=out_specs,
        scratch_shapes=list(scratch),
        compiler_params=pltpu.CompilerParams(vmem_limit_bytes=limit * MIB),
    )


def per_device(
    initial_guess_field,
    medium_label,
    principal_entry_addend,
    linearized_block_weight,
    sample_abscissae,
    singularity_locations,
    basis_normalizers,
    spectral_target,
    quasi_periodic_phase,
):
    points, _, rows, columns = initial_guess_field.shape
    blocks, mats, _ = linearized_block_weight.shape
    tiles = columns // LANES
    planes = 2 * points + 1
    total = rows + 2 * HALO
    count = total // SUB
    names = STEPS + 1
    depth = -(-blocks // SUB) * SUB
    levels = (blocks - 1).bit_length()
    devices = lax.axis_size("gx") * lax.axis_size("gy")
    sds = lambda *shape: jax.ShapeDtypeStruct(shape, F32)

    packed = -(-planes * HALO // SUB) * SUB
    small = [
        principal_entry_addend.T,
        linearized_block_weight.transpose(1, 2, 0),
        sample_abscissae.T,
        singularity_locations.T,
        basis_normalizers.reshape(1, -1),
        spectral_target.reshape(1, -1),
        quasi_periodic_phase,
    ]
    full, *sends = call(
        pack,
        [sds(planes, tiles, total, LANES)]
        + [sds(packed, columns)] * 2
        + [sds(rows, LANES)] * 2
        + [sds(*value.shape) for value in small],
        [HBM] * 9,
        [VMEM] * 12,
        [
            pltpu.VMEM((tiles, rows, LANES), jnp.int32),
            pltpu.SemaphoreType.DMA((tiles * planes + len(small),)),
        ],
        limit=8,
    )(*[pltpu.with_memory_space_constraint(v, pltpu.HBM) for v in (initial_guess_field, medium_label, *small)])
    near_x, far_x, near_y, far_y, *small = sends

    def send(value, axis, pairs):
        return lax.ppermute(value, axis, pairs(axis))

    far_x = send(far_x, "gx", swap_far)
    near_x = send(near_x, "gx", swap_near)
    far_y = send(far_y, "gy", swap_far)
    near_y = send(near_y, "gy", swap_near)

    table, trig, chain, size = call(
        params,
        [
            sds(8, mats, SUB, LANES),
            sds(points, 2, 2, SUB, LANES),
            sds(levels, 2, depth, LANES),
            sds(SUB, LANES),
        ],
        [VMEM] * 7,
        [VMEM] * 4,
        limit=4,
    )(*small)

    own = call(spread, sds(planes, tiles, rows, LANES), [VMEM], VMEM, limit=4)(full)

    near_c, far_c = call(
        pack_corners,
        [sds(2 * HALO, LANES)] * 2,
        [VMEM] * 2,
        [VMEM] * 2,
        [pltpu.VMEM((planes, 2, 2 * HALO, LANES), F32)],
        limit=4,
    )(near_x, far_x)
    far_c = send(far_c, "gy", swap_far)
    near_c = send(near_c, "gy", swap_near)

    narrow = (tiles, count, SUB, LANES)
    cell, b = call(
        stage,
        [sds(6, *narrow), sds(points, 2, *narrow)],
        [VMEM] * 5,
        [VMEM] * 2,
        [
            pltpu.VMEM((planes, tiles, 2 * HALO, LANES), F32),
            pltpu.VMEM((planes, tiles, total, LANES), F32),
        ],
        limit=8,
    )(own, near_x, far_x, table, trig)

    wide = (tiles + 1, count, SUB, LANES)
    out, gram = call(
        solve,
        [sds(STEPS, points, 2, tiles, total, LANES), sds(devices, 1, LANES)],
        [VMEM] * 9,
        [VMEM] * 2,
        [
            pltpu.VMEM((2, total, LANES), F32),
            pltpu.VMEM((planes, total, LANES), F32),
            pltpu.VMEM((6,) + wide[1:], F32),
        ]
        + [pltpu.VMEM((points, 2) + wide, F32)] * 4,
        limit=32,
    )(own, near_y, far_y, near_c, far_c, table, trig, cell, b)

    part = lax.all_to_all(gram, ("gx", "gy"), 0, 0, tiled=True)

    basis, hess = call(
        finish,
        [sds(points, STEPS, 2 * rows, columns), sds(points, STEPS, 2, names)],
        [VMEM] * 5,
        [ANY, VMEM],
        [
            pltpu.VMEM((STEPS, tiles, 2 * rows, LANES), F32),
            pltpu.VMEM((STEPS, columns, LANES), F32),
            pltpu.VMEM((points, STEPS, 2 * rows, columns), F32),
            pltpu.SemaphoreType.DMA((points, STEPS)),
        ],
        limit=16,
    )(own, out, part, chain, size)
    basis = basis.reshape(points, STEPS, 2, rows, columns)
    return basis, hess.transpose(0, 2, 3, 1)


def solution(mesh):
    return jax.shard_map(
        per_device,
        mesh=mesh,
        in_specs=(P(None, None, "gx", "gy"), P("gx", "gy"), P(), P(), P(), P(), P(), P(), P()),
        out_specs=(P(None, None, None, "gx", "gy"), P()),
        check_vma=False,
    )
```

```python
import jax
import jax.numpy as jnp
from jax import lax
from jax.experimental import pallas as pl
from jax.experimental.pallas import tpu as pltpu
from jax.sharding import PartitionSpec as P


STEPS = 3
SWEEPS = 4
HALO = STEPS * SWEEPS
LANES = 128
SUB = 8
SLOT = 16
STRIP = 16
F32 = jnp.float32
VMEM = pl.BlockSpec(memory_space=pltpu.VMEM)
SMEM = pl.BlockSpec(memory_space=pltpu.SMEM)
ANY = pl.BlockSpec(memory_space=pl.ANY)
HBM = pl.BlockSpec(memory_space=pltpu.HBM)
MIB = 1024 * 1024


def even(axis):
    return lax.rem(lax.axis_index(axis), 2) == 0


def swap_near(axis):
    return [(i, i ^ 1) for i in range(lax.axis_size(axis))]


def swap_far(axis):
    n = lax.axis_size(axis)
    return [(i, (i + 1) % n if i % 2 else (i - 1) % n) for i in range(n)]


def cmul(a, b):
    return (a[0] * b[0] - a[1] * b[1], a[0] * b[1] + a[1] * b[0])


def cadd(a, b):
    return (a[0] + b[0], a[1] + b[1])


def csub(a, b):
    return (a[0] - b[0], a[1] - b[1])


def conj_mul(a, b):
    return (a[0] * b[0] + a[1] * b[1], a[0] * b[1] - a[1] * b[0])


def pack_lanes(sides):
    y_even = even("gy")
    shape = sides[0][0].shape
    lane = lax.broadcasted_iota(jnp.int32, shape, 1)
    near_acc = jnp.zeros(shape, F32)
    far_acc = jnp.zeros(shape, F32)
    for plane, (left, right) in enumerate(sides):
        base = plane * SLOT
        keep = (lane >= base) & (lane < base + HALO)
        to_left = jnp.int32(base)
        to_right = jnp.int32((base + HALO) % LANES)
        near = pltpu.roll(jnp.where(y_even, right, left), jnp.where(y_even, to_right, to_left), 1)
        far = pltpu.roll(jnp.where(y_even, left, right), jnp.where(y_even, to_left, to_right), 1)
        near_acc = jnp.where(keep, near, near_acc)
        far_acc = jnp.where(keep, far, far_acc)
    return near_acc, far_acc


def pack_corners(near_x, far_x, near_c, far_c, side_ref):
    planes = side_ref.shape[0]
    columns = near_x.shape[1]
    x_even = even("gx")
    for plane in range(planes):
        span = slice(plane * HALO, (plane + 1) * HALO)
        for side, lanes in enumerate((slice(0, LANES), slice(columns - LANES, columns))):
            near = near_x[span, lanes]
            far = far_x[span, lanes]
            side_ref[plane, side, 0:HALO, :] = jnp.where(x_even, near, far)
            side_ref[plane, side, HALO : 2 * HALO, :] = jnp.where(x_even, far, near)
    near_c[...], far_c[...] = pack_lanes([(side_ref[p, 0], side_ref[p, 1]) for p in range(planes)])


def run_copies(pairs, sem):
    copies = [pltpu.make_async_copy(src, dst, sem.at[n]) for n, (src, dst) in enumerate(pairs)]
    for copy in copies:
        copy.start()
    for copy in copies:
        copy.wait()


def pack_rows(z_hbm, m_hbm, near_x, far_x, strip_ref, label_ref, sem):
    points, _, rows, _ = z_hbm.shape
    pairs = []
    for side, at in enumerate((0, rows - STRIP)):
        span = pl.ds(at, STRIP)
        for plane in range(2 * points):
            src = z_hbm.at[plane // 2, plane % 2, span, :]
            pairs.append((src, strip_ref.at[plane, side]))
        pairs.append((m_hbm.at[span, :], label_ref.at[side]))
    run_copies(pairs, sem)
    x_even = even("gx")
    for plane in range(2 * points + 1):
        if plane < 2 * points:
            top = strip_ref[plane, 0, 0:HALO, :]
            bottom = strip_ref[plane, 1, STRIP - HALO : STRIP, :]
        else:
            top = label_ref[0, 0:HALO, :].astype(F32)
            bottom = label_ref[1, STRIP - HALO : STRIP, :].astype(F32)
        span = slice(plane * HALO, (plane + 1) * HALO)
        near_x[span, :] = jnp.where(x_even, bottom, top)
        far_x[span, :] = jnp.where(x_even, top, bottom)


def load(z_hbm, m_hbm, a_hbm, w_hbm, node_hbm, pole_hbm, scale_hbm, target_hbm, phase_hbm,
         full_ref, near_y, far_y,
         a_ref, w_ref, node_ref, pole_ref, scale_ref, target_ref, phase_ref, label_ref, sem):
    points, _, _, columns = z_hbm.shape
    tiles = columns // LANES
    planes = 2 * points + 1
    pairs = []
    for t in range(tiles):
        lanes = pl.ds(t * LANES, LANES)
        for plane in range(2 * points):
            src = z_hbm.at[plane // 2, plane % 2, :, lanes]
            pairs.append((src, full_ref.at[plane, t]))
        pairs.append((m_hbm.at[:, lanes], label_ref.at[t]))
    pairs += [(a_hbm, a_ref), (w_hbm, w_ref), (node_hbm, node_ref), (pole_hbm, pole_ref)]
    pairs += [(scale_hbm, scale_ref), (target_hbm, target_ref), (phase_hbm, phase_ref)]
    run_copies(pairs, sem)
    for t in range(tiles):
        full_ref[planes - 1, t] = label_ref[t].astype(F32)
    sides = [(full_ref[p, 0], full_ref[p, tiles - 1]) for p in range(planes)]
    near_y[...], far_y[...] = pack_lanes(sides)


def params(a_ref, w_ref, node_ref, pole_ref, scale_ref, target_ref, phase_ref,
           table_ref, trig_ref, chain_ref, size_ref):
    shape = (SUB, LANES)

    def full(value):
        return jnp.broadcast_to(value, shape)

    mats = a_ref.shape[1]
    totals = node_ref.shape[1]
    target = (target_ref[:, 0:1], target_ref[:, 1:2])
    gap = csub(target, (node_ref[0:1, :], node_ref[1:2, :]))
    pole = (pole_ref[0:1, :], pole_ref[1:2, :])
    pole_size = pole[0] * pole[0] + pole[1] * pole[1]
    quotient = conj_mul(pole, target)
    quotient = (quotient[0] / pole_size, quotient[1] / pole_size)
    scale = scale_ref[...]
    lower = (scale * (1.0 - quotient[0]), -scale * quotient[1])
    lower_size = lower[0] * lower[0] + lower[1] * lower[1]
    factor = conj_mul(lower, gap)
    factor = (factor[0] / lower_size, factor[1] / lower_size)
    steps = [tuple(full(factor[c][:, j : j + 1]) for c in range(2)) for j in range(totals)]
    zero = jnp.zeros(shape, F32)
    lane = lax.broadcasted_iota(jnp.int32, shape, 1)
    power = (jnp.ones(shape, F32), zero)
    size = jnp.ones(shape, F32)
    powers = [jnp.where(lane == 0, power[0], zero), zero]
    for b in range(1, totals + 1):
        power = cmul(power, steps[b - 1])
        size = size + (power[0] * power[0] + power[1] * power[1])
        for c in range(2):
            powers[c] = jnp.where(lane == b, power[c], powers[c])
    gamma = jnp.sqrt(size)
    size_ref[...] = gamma
    blocks = totals + 1
    line = tuple((powers[c] / gamma)[0:1, :blocks] for c in range(2))
    order = lax.broadcasted_iota(jnp.int32, (1, blocks), 1).astype(F32)
    for m in range(mats):
        center = 4.0 + full(a_ref[0:1, m : m + 1])
        side = full(a_ref[1:2, m : m + 1])
        inverse_size = center * center + side * side
        inverse = (center / inverse_size, -side / inverse_size)
        w = (w_ref[m, 0:1, :], w_ref[m, 1:2, :])
        first = (full(w[0][:, 0:1]), full(w[1][:, 0:1]))
        product = cmul(w, line)
        a_weight = tuple(full(jnp.sum(p, axis=1, keepdims=True)) for p in product)
        b_weight = tuple(full(jnp.sum(p * order, axis=1, keepdims=True)) for p in product)
        b_weight = (b_weight[0] / gamma, b_weight[1] / gamma)
        entries = (inverse, cmul(inverse, first), cmul(inverse, a_weight), cmul(inverse, b_weight))
        for e, (re, im) in enumerate(entries):
            table_ref[2 * e, m] = re
            table_ref[2 * e + 1, m] = im
    for k in range(phase_ref.shape[0]):
        for axis in range(2):
            angle = full(phase_ref[k : k + 1, axis : axis + 1])
            trig_ref[k, axis, 0] = jnp.cos(angle)
            trig_ref[k, axis, 1] = jnp.sin(angle)
    depth = chain_ref.shape[2]
    row = lax.broadcasted_iota(jnp.int32, shape, 0)
    tiles = [[], []]
    for c in range(2):
        for t in range(depth // SUB):
            value = zero
            for r in range(SUB):
                b = t * SUB + r
                if 1 <= b <= totals:
                    value = jnp.where(row == r, steps[b - 1][c], value)
            tiles[c].append(value)
    step = tuple(jnp.concatenate(tile, 0) for tile in tiles)
    for s in range(chain_ref.shape[0]):
        chain_ref[s, 0] = step[0]
        chain_ref[s, 1] = step[1]
        moved = (pltpu.roll(step[0], 1 << s, 0), pltpu.roll(step[1], 1 << s, 0))
        step = cmul(step, moved)


def spread_lanes(tiles):
    count = len(tiles)
    shape = tiles[0].shape
    lane = lax.broadcasted_iota(jnp.int32, shape, 1)
    owner = lane // (LANES // count)
    result = []
    for j in range(count):
        index = lax.rem(lane * count + j, LANES)
        value = jnp.take_along_axis(tiles[0], index, axis=1)
        for t in range(1, count):
            value = jnp.where(owner == t, jnp.take_along_axis(tiles[t], index, axis=1), value)
        result.append(value)
    return result


def spread(full_ref, own_ref):
    planes, tiles, rows, _ = own_ref.shape
    for plane in range(planes):
        for r in range(0, rows, SUB):
            values = spread_lanes([full_ref[plane, t, r : r + SUB, :] for t in range(tiles)])
            for j, value in enumerate(values):
                own_ref[plane, j, r : r + SUB, :] = value


def picker(label, table_ref):
    mats = table_ref.shape[1]
    picks = [label == float(m) for m in range(1, mats)]

    def pick(e):
        value = table_ref[e, 0]
        for m in range(1, mats):
            value = jnp.where(picks[m - 1], table_ref[e, m], value)
        return value

    return pick


def ends(axis):
    first = (lax.axis_index(axis) == 0).astype(F32)
    last = (lax.axis_index(axis) == lax.axis_size(axis) - 1).astype(F32)
    return first, last


def row_turns(trig_ref, k):
    first, last = ends("gx")
    low = lax.broadcasted_iota(jnp.int32, (2 * HALO, LANES), 0) < HALO
    edge = jnp.where(low, last, first) > 0.5
    sine = trig_ref[k, 0, 1][0:1, :]
    co = jnp.where(edge, trig_ref[k, 0, 0][0:1, :], 1.0)
    return co, jnp.where(edge, jnp.where(low, sine, -sine), 0.0)


def stage(own_ref, near_x, far_x, table_ref, trig_ref, cell_ref, b_ref, raw_ref, work_ref):
    planes, tiles, rows, _ = own_ref.shape
    points = planes // 2
    total = rows + 2 * HALO
    count = total // SUB
    x_even = even("gx")
    for plane in range(planes):
        span = slice(plane * HALO, (plane + 1) * HALO)
        for t in range(tiles):
            lanes = slice(t * LANES, (t + 1) * LANES)
            near = near_x[span, lanes]
            far = far_x[span, lanes]
            raw_ref[plane, t, 0:HALO, :] = jnp.where(x_even, near, far)
            raw_ref[plane, t, HALO : 2 * HALO, :] = jnp.where(x_even, far, near)
            work_ref[plane, t, 0:rows, :] = own_ref[plane, t]
    for k in range(points):
        turn = row_turns(trig_ref, k)
        for t in range(tiles):
            turned = cmul((raw_ref[2 * k, t], raw_ref[2 * k + 1, t]), turn)
            raw_ref[2 * k, t] = turned[0]
            raw_ref[2 * k + 1, t] = turned[1]
    for plane in range(planes):
        for r in range(0, 2 * HALO, SUB):
            values = spread_lanes([raw_ref[plane, t, r : r + SUB, :] for t in range(tiles)])
            for j, value in enumerate(values):
                work_ref[plane, j, rows + r : rows + r + SUB, :] = value
    for j in range(tiles):
        for v in range(count):
            span = pl.ds(v, SUB, stride=count)
            pick = picker(work_ref[planes - 1, j, span, :], table_ref)
            for n, e in enumerate((0, 1, 4, 5, 6, 7)):
                cell_ref[n, j, v] = pick(e)
            weight = (pick(2), pick(3))
            for k in range(points):
                z = (work_ref[2 * k, j, span, :], work_ref[2 * k + 1, j, span, :])
                for c, value in enumerate(cmul(weight, z)):
                    b_ref[k, c, j, v] = value


def solve(own_ref, near_y, far_y, near_c, far_c, table_ref, trig_ref, cell_own, b_own,
          out_ref, gram_ref, edge_ref, halo_ref, cell_halo, b_ref, x_ref, w_ref, keep_ref):
    planes, tiles, rows, _ = own_ref.shape
    points = planes // 2
    total = rows + 2 * HALO
    count = total // SUB
    y_even = even("gy")
    for side in range(2):
        keep = y_even if side == 0 else jnp.logical_not(y_even)
        edge_ref[side, 0:rows, :] = jnp.where(keep, near_y[...], far_y[...])
        edge_ref[side, rows:total, :] = jnp.where(keep, near_c[...], far_c[...])
    lane = lax.broadcasted_iota(jnp.int32, (total, LANES), 1)
    is_right = lane < HALO
    is_left = lane >= LANES - HALO
    right_src = edge_ref[0]
    left_src = edge_ref[1]
    for plane in range(planes):
        right = pltpu.roll(right_src, (LANES - plane * SLOT) % LANES, 1)
        left = pltpu.roll(left_src, (LANES - HALO - plane * SLOT) % LANES, 1)
        halo_ref[plane] = jnp.where(is_right, right, jnp.where(is_left, left, 0.0))
    first, last = ends("gy")
    y_edge = jnp.where(is_right, last, jnp.where(is_left, first, 0.0)) > 0.5
    for k in range(points):
        turned = cmul(
            (halo_ref[2 * k, rows:total, :], halo_ref[2 * k + 1, rows:total, :]),
            row_turns(trig_ref, k),
        )
        halo_ref[2 * k, rows:total, :] = turned[0]
        halo_ref[2 * k + 1, rows:total, :] = turned[1]
        sine = trig_ref[k, 1, 1][0:1, :]
        co = jnp.where(y_edge, trig_ref[k, 1, 0][0:1, :], 1.0)
        si = jnp.where(y_edge, jnp.where(is_right, sine, -sine), 0.0)
        turned = cmul((halo_ref[2 * k], halo_ref[2 * k + 1]), (co, si))
        halo_ref[2 * k] = turned[0]
        halo_ref[2 * k + 1] = turned[1]
    for v in range(count):
        span = pl.ds(v, SUB, stride=count)
        pick = picker(halo_ref[planes - 1, span, :], table_ref)
        for n, e in enumerate((0, 1, 4, 5, 6, 7)):
            cell_halo[n, v] = pick(e)
        weight = (pick(2), pick(3))
        for k in range(points):
            z = (halo_ref[2 * k, span, :], halo_ref[2 * k + 1, span, :])
            for c, value in enumerate(cmul(weight, z)):
                b_ref[k, c, tiles, v] = value
                x_ref[k, c, tiles, v] = value
                for t in range(tiles):
                    own = b_own[k, c, t, v]
                    b_ref[k, c, t, v] = own
                    x_ref[k, c, t, v] = own

    def cell(e, t, v):
        return cell_own[e, t, v] if t < tiles else cell_halo[e, v]

    lane8 = lax.broadcasted_iota(jnp.int32, (SUB, LANES), 1)
    at_first = lane8 == 0
    at_last = lane8 == LANES - 1

    def sweep(src_ref, dst_ref):
        for k in range(points):
            for v in range(count):
                sides = []
                for c in range(2):
                    x = [src_ref[k, c, t, v] for t in range(tiles + 1)]
                    last_on = pltpu.roll(x[tiles - 1], 1, 1)
                    halo_on = pltpu.roll(x[tiles], 1, 1)
                    first_back = pltpu.roll(x[0], LANES - 1, 1)
                    halo_back = pltpu.roll(x[tiles], LANES - 1, 1)
                    left = [jnp.where(at_first, halo_on, last_on)] + x[: tiles - 1]
                    right = x[1:tiles] + [jnp.where(at_last, halo_back, first_back)]
                    side = [a + b for a, b in zip(left, right)]
                    one = jnp.where(at_first, last_on, halo_on)
                    two = jnp.where(at_last, first_back, halo_back)
                    sides.append(side + [one + two])
                for t in range(tiles + 1):
                    n = []
                    for c in range(2):
                        if v > 0:
                            up = src_ref[k, c, t, v - 1]
                        else:
                            up = pltpu.roll(src_ref[k, c, t, count - 1], 1, 0)
                        if v < count - 1:
                            down = src_ref[k, c, t, v + 1]
                        else:
                            down = pltpu.roll(src_ref[k, c, t, 0], SUB - 1, 0)
                        n.append(sides[c][t] + (up + down))
                    n = cmul((cell(0, t, v), cell(1, t, v)), n)
                    for c in range(2):
                        dst_ref[k, c, t, v] = b_ref[k, c, t, v] + n[c]

    def pair(i, carry):
        sweep(x_ref, w_ref)
        sweep(w_ref, x_ref)
        return carry

    for s in range(STEPS):
        lax.fori_loop(0, SWEEPS // 2, pair, 0)
        for k in range(points):
            for t in range(tiles + 1):
                for v in range(count):
                    y = (x_ref[k, 0, t, v], x_ref[k, 1, t, v])
                    if t < tiles:
                        for c in range(2):
                            out_ref[s, k, c, t, pl.ds(v, SUB, stride=count), :] = y[c]
                    if s < STEPS - 1:
                        b = cmul((cell(2, t, v), cell(3, t, v)), y)
                        if s == 0:
                            keep = cmul((cell(4, t, v), cell(5, t, v)), y)
                            for c in range(2):
                                keep_ref[k, c, t, v] = keep[c]
                        else:
                            b = cadd(b, (keep_ref[k, 0, t, v], keep_ref[k, 1, t, v]))
                        for c in range(2):
                            b_ref[k, c, t, v] = b[c]
                            x_ref[k, c, t, v] = b[c]

    names = STEPS + 1
    zero = jnp.zeros((SUB, LANES), F32)
    line = jnp.zeros((1, LANES), F32)
    lane1 = lax.broadcasted_iota(jnp.int32, (1, LANES), 1)
    entries = [(i, j) for i in range(names) for j in range(i, names)]
    for k in range(points):

        def gather(r, accs):
            accs = list(accs)
            span = pl.ds(pl.multiple_of(r * SUB, SUB), SUB)
            for t in range(tiles):
                fields = [(own_ref[2 * k, t, span, :], own_ref[2 * k + 1, t, span, :])]
                for s in range(STEPS):
                    fields.append((out_ref[s, k, 0, t, span, :], out_ref[s, k, 1, t, span, :]))
                at = 0
                for i, j in entries:
                    if i == j:
                        a = fields[i]
                        accs[at] = accs[at] + (a[0] * a[0] + a[1] * a[1])
                        at += 1
                    else:
                        product = conj_mul(fields[i], fields[j])
                        accs[at] = accs[at] + product[0]
                        accs[at + 1] = accs[at + 1] + product[1]
                        at += 2
            return tuple(accs)

        accs = lax.fori_loop(0, rows // SUB, gather, (zero,) * (names * names))
        for e, acc in enumerate(accs):
            value = jnp.sum(jnp.sum(acc, axis=0, keepdims=True), axis=1, keepdims=True)
            line = jnp.where(lane1 == k * names * names + e, value, line)
    gram_ref[...] = jnp.broadcast_to(line[None], gram_ref.shape)


def finish(own_ref, out_ref, part_ref, chain_ref, size_ref, basis_ref, hess_out,
           found_ref, turn_ref, done_ref, hess_ref, sem, hess_sem):
    planes, tiles, rows, _ = own_ref.shape
    points = planes // 2
    names = STEPS + 1
    shape = (SUB, LANES)
    line = jnp.sum(part_ref[:, 0, :], axis=0, keepdims=True)
    uppers = []
    inverses = []
    copies = []
    for k in range(points):
        base = k * names * names
        gram = {}
        at = base
        for i in range(names):
            for j in range(i, names):
                width = 1 if i == j else 2
                gram[i, j] = tuple(
                    jnp.broadcast_to(line[:, at + c : at + c + 1], shape) for c in range(width)
                )
                at += width
        upper = {}
        inv = []
        for i in range(names):
            pivot = gram[i, i][0]
            for l in range(i):
                pivot = pivot - (upper[l, i][0] * upper[l, i][0] + upper[l, i][1] * upper[l, i][1])
            root = jnp.sqrt(pivot)
            upper[i, i] = root
            inv.append(1.0 / root)
            for j in range(i + 1, names):
                value = gram[i, j]
                for l in range(i):
                    value = csub(value, conj_mul(upper[l, i], upper[l, j]))
                upper[i, j] = (value[0] * inv[i], value[1] * inv[i])
        uppers.append(upper)
        inverses.append(inv)

    def combine(k, r):
        upper = uppers[k]
        inv = inverses[k]
        span = slice(r * SUB, (r + 1) * SUB)
        for t in range(tiles):
            fields = [(own_ref[2 * k, t, span, :], own_ref[2 * k + 1, t, span, :])]
            for s in range(STEPS):
                fields.append((out_ref[s, k, 0, t, span, :], out_ref[s, k, 1, t, span, :]))
            found = []
            for i in range(names):
                value = fields[i]
                for l in range(i):
                    value = csub(value, cmul(upper[l, i], found[l]))
                value = (value[0] * inv[i], value[1] * inv[i])
                found.append(value)
                if i > 0:
                    for c in range(2):
                        place = slice(c * rows + r * SUB, c * rows + (r + 1) * SUB)
                        found_ref[k, i - 1, t, place, :] = value[c]

    piece = 32
    for k in range(points):
        for r in range(rows // SUB):
            combine(k, r)
        for i in range(STEPS):
            for n in range(0, 2 * rows, LANES):
                for t in range(tiles):
                    turned = found_ref[k, i, t, n : n + LANES, :].T
                    turn_ref[k, i, pl.ds(t, LANES, stride=tiles), :] = turned
                for t in range(tiles):
                    lanes = slice(t * LANES, (t + 1) * LANES)
                    done_ref[k, i, n : n + LANES, lanes] = turn_ref[k, i, lanes, :].T
            for at, n in enumerate(range(0, 2 * rows, piece)):
                part = pl.ds(n, piece)
                copy = pltpu.make_async_copy(
                    done_ref.at[k, i, part, :], basis_ref.at[k, i, part, :], sem.at[k, i, at]
                )
                copy.start()
                copies.append(copy)

    lane = lax.broadcasted_iota(jnp.int32, shape, 1)

    def mixed(pick):
        value = pick(0)
        for k in range(1, points):
            value = jnp.where(lane == k, pick(k), value)
        return value

    gamma = size_ref[...]
    inv0 = mixed(lambda k: inverses[k][0])
    column = []
    for j in range(1, names):
        entry = []
        for i in range(j):
            entry.append(tuple(mixed(lambda k: uppers[k][i, j][c]) * inv0 for c in range(2)))
        entry.append((mixed(lambda k: uppers[k][j, j]) * inv0, jnp.zeros(shape, F32)))
        column.append(entry)

    depth = chain_ref.shape[2]
    row = lax.broadcasted_iota(jnp.int32, (depth, LANES), 0)
    tall = lambda value: jnp.broadcast_to(value[0:1], (depth, LANES))
    nil = jnp.zeros((depth, LANES), F32)
    at_top = row == 0
    basis_u = [[(jnp.where(at_top, 1.0, 0.0), nil)]]
    hess = {}
    coords = []
    mus = []
    for k in range(STEPS):
        active = k + 1
        if k == 0:
            found = column[0]
        elif k == 1:
            found = []
            for i in range(3):
                value = (column[1][i][0] * gamma, column[1][i][1] * gamma)
                if i < 2:
                    value = csub(value, cmul(hess[0, 0], coords[0][i]))
                found.append((value[0] / mus[0], value[1] / mus[0]))
        else:
            found = []
            scale = gamma / mus[0]
            for i in range(4):
                value = (column[2][i][0] * gamma, column[2][i][1] * gamma)
                if i < 3:
                    value = csub(value, cmul(hess[0, 0], column[1][i]))
                value = (value[0] * scale, value[1] * scale)
                if i < 2:
                    value = csub(value, cmul(hess[0, 1], coords[0][i]))
                if i < 3:
                    value = csub(value, cmul(hess[1, 1], coords[1][i]))
                found.append((value[0] / mus[1], value[1] / mus[1]))
        coords.append(found)
        current = basis_u[k]
        x = []
        for i in range(active + 1):
            old = current[i] if i < len(current) else (nil, nil)
            value = tuple(jnp.where(at_top, tall(found[i][c]), old[c]) for c in range(2))
            for s in range(chain_ref.shape[0]):
                step = (chain_ref[s, 0], chain_ref[s, 1])
                moved = tuple(pltpu.roll(value[c], 1 << s, 0) for c in range(2))
                value = cadd(value, cmul(step, moved))
            x.append(value)
        total_t = [None] * active
        for turn in range(2):
            inner = []
            for j in range(active):
                acc = (nil, nil)
                for i in range(len(basis_u[j])):
                    acc = cadd(acc, conj_mul(basis_u[j][i], x[i]))
                inner.append(tuple(jnp.sum(acc[c], axis=0, keepdims=True) for c in range(2)))
            for j in range(active):
                for i in range(len(basis_u[j])):
                    x[i] = csub(x[i], cmul(inner[j], basis_u[j][i]))
                total_t[j] = inner[j] if turn == 0 else cadd(total_t[j], inner[j])
        square = nil
        for value in x:
            square = square + (value[0] * value[0] + value[1] * value[1])
        mu = jnp.sqrt(jnp.sum(square, axis=0, keepdims=True))
        mus.append(jnp.broadcast_to(mu, shape))
        basis_u.append([(value[0] / mu, value[1] / mu) for value in x])
        for j in range(active):
            hess[j, k] = tuple(jnp.broadcast_to(total_t[j][c], shape) for c in range(2))
    part_row = lax.broadcasted_iota(jnp.int32, (2, names), 0)
    part_lane = lax.broadcasted_iota(jnp.int32, (2, names), 1)
    for p in range(points):
        for k in range(STEPS):
            value = jnp.zeros((2, names), F32)
            for j in range(k + 2):
                parts = hess[j, k] if j <= k else (mus[k],)
                for c, entry in enumerate(parts):
                    here = (part_row == c) & (part_lane == j)
                    value = jnp.where(here, entry[0:1, p : p + 1], value)
            hess_ref[p, k] = value
    copy = pltpu.make_async_copy(hess_ref, hess_out, hess_sem)
    copy.start()
    copies.append(copy)
    for copy in copies:
        copy.wait()


def call(body, outs, specs, out_specs, scratch=(), limit=16):
    return pl.pallas_call(
        body,
        out_shape=outs,
        in_specs=specs,
        out_specs=out_specs,
        scratch_shapes=list(scratch),
        compiler_params=pltpu.CompilerParams(vmem_limit_bytes=limit * MIB),
    )


def per_device(
    initial_guess_field,
    medium_label,
    principal_entry_addend,
    linearized_block_weight,
    sample_abscissae,
    singularity_locations,
    basis_normalizers,
    spectral_target,
    quasi_periodic_phase,
):
    points, _, rows, columns = initial_guess_field.shape
    blocks, mats, _ = linearized_block_weight.shape
    tiles = columns // LANES
    planes = 2 * points + 1
    total = rows + 2 * HALO
    count = total // SUB
    names = STEPS + 1
    depth = -(-blocks // SUB) * SUB
    levels = (blocks - 1).bit_length()
    devices = lax.axis_size("gx") * lax.axis_size("gy")
    sds = lambda *shape: jax.ShapeDtypeStruct(shape, F32)

    packed = -(-planes * HALO // SUB) * SUB
    small = [
        principal_entry_addend.T,
        linearized_block_weight.transpose(1, 2, 0),
        sample_abscissae.T,
        singularity_locations.T,
        basis_normalizers.reshape(1, -1),
        spectral_target.reshape(1, -1),
        quasi_periodic_phase,
    ]
    hbm = lambda v: pltpu.with_memory_space_constraint(v, pltpu.HBM)
    field = hbm(initial_guess_field)
    label = hbm(medium_label)
    near_x, far_x = call(
        pack_rows,
        [sds(packed, columns)] * 2,
        [HBM] * 2,
        [VMEM] * 2,
        [
            pltpu.VMEM((2 * points, 2, STRIP, columns), F32),
            pltpu.VMEM((2, STRIP, columns), jnp.int32),
            pltpu.SemaphoreType.DMA((2 * planes,)),
        ],
        limit=8,
    )(field, label)

    def send(value, axis, pairs):
        return lax.ppermute(value, axis, pairs(axis))

    far_x = send(far_x, "gx", swap_far)
    near_x = send(near_x, "gx", swap_near)
    full, near_y, far_y, *small = call(
        load,
        [sds(planes, tiles, rows, LANES)]
        + [sds(rows, LANES)] * 2
        + [sds(*value.shape) for value in small],
        [HBM] * 9,
        [VMEM] * 10,
        [
            pltpu.VMEM((tiles, rows, LANES), jnp.int32),
            pltpu.SemaphoreType.DMA((tiles * planes + len(small),)),
        ],
        limit=8,
    )(field, label, *[hbm(v) for v in small])
    far_y = send(far_y, "gy", swap_far)
    near_y = send(near_y, "gy", swap_near)

    table, trig, chain, size = call(
        params,
        [
            sds(8, mats, SUB, LANES),
            sds(points, 2, 2, SUB, LANES),
            sds(levels, 2, depth, LANES),
            sds(SUB, LANES),
        ],
        [VMEM] * 7,
        [VMEM] * 4,
        limit=4,
    )(*small)

    own = call(spread, sds(planes, tiles, rows, LANES), [VMEM], VMEM, limit=4)(full)

    near_c, far_c = call(
        pack_corners,
        [sds(2 * HALO, LANES)] * 2,
        [VMEM] * 2,
        [VMEM] * 2,
        [pltpu.VMEM((planes, 2, 2 * HALO, LANES), F32)],
        limit=4,
    )(near_x, far_x)
    far_c = send(far_c, "gy", swap_far)
    near_c = send(near_c, "gy", swap_near)

    narrow = (tiles, count, SUB, LANES)
    cell, b = call(
        stage,
        [sds(6, *narrow), sds(points, 2, *narrow)],
        [VMEM] * 5,
        [VMEM] * 2,
        [
            pltpu.VMEM((planes, tiles, 2 * HALO, LANES), F32),
            pltpu.VMEM((planes, tiles, total, LANES), F32),
        ],
        limit=8,
    )(own, near_x, far_x, table, trig)

    wide = (tiles + 1, count, SUB, LANES)
    out, gram = call(
        solve,
        [sds(STEPS, points, 2, tiles, total, LANES), sds(devices, 1, LANES)],
        [VMEM] * 9,
        [VMEM] * 2,
        [
            pltpu.VMEM((2, total, LANES), F32),
            pltpu.VMEM((planes, total, LANES), F32),
            pltpu.VMEM((6,) + wide[1:], F32),
        ]
        + [pltpu.VMEM((points, 2) + wide, F32)] * 4,
        limit=32,
    )(own, near_y, far_y, near_c, far_c, table, trig, cell, b)

    part = lax.all_to_all(gram, ("gx", "gy"), 0, 0, tiled=True)

    basis, hess = call(
        finish,
        [sds(points, STEPS, 2 * rows, columns), sds(points, STEPS, 2, names)],
        [VMEM] * 5,
        [ANY, ANY],
        [
            pltpu.VMEM((points, STEPS, tiles, 2 * rows, LANES), F32),
            pltpu.VMEM((points, STEPS, columns, LANES), F32),
            pltpu.VMEM((points, STEPS, 2 * rows, columns), F32),
            pltpu.VMEM((points, STEPS, 2, names), F32),
            pltpu.SemaphoreType.DMA((points, STEPS, 2 * rows // 32)),
            pltpu.SemaphoreType.DMA,
        ],
        limit=16,
    )(own, out, part, chain, size)
    basis = basis.reshape(points, STEPS, 2, rows, columns)
    return basis, hess.transpose(0, 2, 3, 1)


def solution(mesh):
    return jax.shard_map(
        per_device,
        mesh=mesh,
        in_specs=(P(None, None, "gx", "gy"), P("gx", "gy"), P(), P(), P(), P(), P(), P(), P()),
        out_specs=(P(None, None, None, "gx", "gy"), P()),
        check_vma=False,
    )
```

```python
import jax
import jax.numpy as jnp
from jax import lax
from jax.experimental import pallas as pl
from jax.experimental.pallas import tpu as pltpu
from jax.sharding import PartitionSpec as P


STEPS = 3
SWEEPS = 4
HALO = STEPS * SWEEPS
LANES = 128
SUB = 8
SLOT = 16
STRIP = 16
F32 = jnp.float32
VMEM = pl.BlockSpec(memory_space=pltpu.VMEM)
SMEM = pl.BlockSpec(memory_space=pltpu.SMEM)
ANY = pl.BlockSpec(memory_space=pl.ANY)
HBM = pl.BlockSpec(memory_space=pltpu.HBM)
MIB = 1024 * 1024


def even(axis):
    return lax.rem(lax.axis_index(axis), 2) == 0


def swap_near(axis):
    return [(i, i ^ 1) for i in range(lax.axis_size(axis))]


def swap_far(axis):
    n = lax.axis_size(axis)
    return [(i, (i + 1) % n if i % 2 else (i - 1) % n) for i in range(n)]


def cmul(a, b):
    return (a[0] * b[0] - a[1] * b[1], a[0] * b[1] + a[1] * b[0])


def cadd(a, b):
    return (a[0] + b[0], a[1] + b[1])


def csub(a, b):
    return (a[0] - b[0], a[1] - b[1])


def conj_mul(a, b):
    return (a[0] * b[0] + a[1] * b[1], a[0] * b[1] - a[1] * b[0])


def pack_lanes(sides):
    y_even = even("gy")
    shape = sides[0][0].shape
    lane = lax.broadcasted_iota(jnp.int32, shape, 1)
    near_acc = jnp.zeros(shape, F32)
    far_acc = jnp.zeros(shape, F32)
    for plane, (left, right) in enumerate(sides):
        base = plane * SLOT
        keep = (lane >= base) & (lane < base + HALO)
        to_left = jnp.int32(base)
        to_right = jnp.int32((base + HALO) % LANES)
        near = pltpu.roll(jnp.where(y_even, right, left), jnp.where(y_even, to_right, to_left), 1)
        far = pltpu.roll(jnp.where(y_even, left, right), jnp.where(y_even, to_left, to_right), 1)
        near_acc = jnp.where(keep, near, near_acc)
        far_acc = jnp.where(keep, far, far_acc)
    return near_acc, far_acc


def pack_corners(near_x, far_x, near_c, far_c, side_ref):
    planes = side_ref.shape[0]
    columns = near_x.shape[1]
    x_even = even("gx")
    for plane in range(planes):
        span = slice(plane * HALO, (plane + 1) * HALO)
        for side, lanes in enumerate((slice(0, LANES), slice(columns - LANES, columns))):
            near = near_x[span, lanes]
            far = far_x[span, lanes]
            side_ref[plane, side, 0:HALO, :] = jnp.where(x_even, near, far)
            side_ref[plane, side, HALO : 2 * HALO, :] = jnp.where(x_even, far, near)
    near_c[...], far_c[...] = pack_lanes([(side_ref[p, 0], side_ref[p, 1]) for p in range(planes)])


def run_copies(pairs, sem):
    copies = [pltpu.make_async_copy(src, dst, sem.at[n]) for n, (src, dst) in enumerate(pairs)]
    for copy in copies:
        copy.start()
    for copy in copies:
        copy.wait()


def pack_rows(z_hbm, m_hbm, near_x, far_x, strip_ref, label_ref, sem):
    points, _, rows, _ = z_hbm.shape
    pairs = []
    for side, at in enumerate((0, rows - STRIP)):
        span = pl.ds(at, STRIP)
        for plane in range(2 * points):
            src = z_hbm.at[plane // 2, plane % 2, span, :]
            pairs.append((src, strip_ref.at[plane, side]))
        pairs.append((m_hbm.at[span, :], label_ref.at[side]))
    run_copies(pairs, sem)
    x_even = even("gx")
    for plane in range(2 * points + 1):
        if plane < 2 * points:
            top = strip_ref[plane, 0, 0:HALO, :]
            bottom = strip_ref[plane, 1, STRIP - HALO : STRIP, :]
        else:
            top = label_ref[0, 0:HALO, :].astype(F32)
            bottom = label_ref[1, STRIP - HALO : STRIP, :].astype(F32)
        span = slice(plane * HALO, (plane + 1) * HALO)
        near_x[span, :] = jnp.where(x_even, bottom, top)
        far_x[span, :] = jnp.where(x_even, top, bottom)


def load(z_hbm, m_hbm, a_hbm, w_hbm, node_hbm, pole_hbm, scale_hbm, target_hbm, phase_hbm,
         full_ref, near_y, far_y,
         a_ref, w_ref, node_ref, pole_ref, scale_ref, target_ref, phase_ref, label_ref, sem):
    points, _, _, columns = z_hbm.shape
    tiles = columns // LANES
    planes = 2 * points + 1
    pairs = []
    for t in range(tiles):
        lanes = pl.ds(t * LANES, LANES)
        for plane in range(2 * points):
            src = z_hbm.at[plane // 2, plane % 2, :, lanes]
            pairs.append((src, full_ref.at[plane, t]))
        pairs.append((m_hbm.at[:, lanes], label_ref.at[t]))
    pairs += [(a_hbm, a_ref), (w_hbm, w_ref), (node_hbm, node_ref), (pole_hbm, pole_ref)]
    pairs += [(scale_hbm, scale_ref), (target_hbm, target_ref), (phase_hbm, phase_ref)]
    run_copies(pairs, sem)
    for t in range(tiles):
        full_ref[planes - 1, t] = label_ref[t].astype(F32)
    sides = [(full_ref[p, 0], full_ref[p, tiles - 1]) for p in range(planes)]
    near_y[...], far_y[...] = pack_lanes(sides)


def params(a_ref, w_ref, node_ref, pole_ref, scale_ref, target_ref, phase_ref,
           table_ref, trig_ref, chain_ref, size_ref):
    shape = (SUB, LANES)

    def full(value):
        return jnp.broadcast_to(value, shape)

    mats = a_ref.shape[1]
    totals = node_ref.shape[1]
    target = (target_ref[:, 0:1], target_ref[:, 1:2])
    gap = csub(target, (node_ref[0:1, :], node_ref[1:2, :]))
    pole = (pole_ref[0:1, :], pole_ref[1:2, :])
    pole_size = pole[0] * pole[0] + pole[1] * pole[1]
    quotient = conj_mul(pole, target)
    quotient = (quotient[0] / pole_size, quotient[1] / pole_size)
    scale = scale_ref[...]
    lower = (scale * (1.0 - quotient[0]), -scale * quotient[1])
    lower_size = lower[0] * lower[0] + lower[1] * lower[1]
    factor = conj_mul(lower, gap)
    factor = (factor[0] / lower_size, factor[1] / lower_size)
    steps = [tuple(full(factor[c][:, j : j + 1]) for c in range(2)) for j in range(totals)]
    zero = jnp.zeros(shape, F32)
    lane = lax.broadcasted_iota(jnp.int32, shape, 1)
    power = (jnp.ones(shape, F32), zero)
    size = jnp.ones(shape, F32)
    powers = [jnp.where(lane == 0, power[0], zero), zero]
    for b in range(1, totals + 1):
        power = cmul(power, steps[b - 1])
        size = size + (power[0] * power[0] + power[1] * power[1])
        for c in range(2):
            powers[c] = jnp.where(lane == b, power[c], powers[c])
    gamma = jnp.sqrt(size)
    size_ref[...] = gamma
    blocks = totals + 1
    line = tuple((powers[c] / gamma)[0:1, :blocks] for c in range(2))
    order = lax.broadcasted_iota(jnp.int32, (1, blocks), 1).astype(F32)
    for m in range(mats):
        center = 4.0 + full(a_ref[0:1, m : m + 1])
        side = full(a_ref[1:2, m : m + 1])
        inverse_size = center * center + side * side
        inverse = (center / inverse_size, -side / inverse_size)
        w = (w_ref[m, 0:1, :], w_ref[m, 1:2, :])
        first = (full(w[0][:, 0:1]), full(w[1][:, 0:1]))
        product = cmul(w, line)
        a_weight = tuple(full(jnp.sum(p, axis=1, keepdims=True)) for p in product)
        b_weight = tuple(full(jnp.sum(p * order, axis=1, keepdims=True)) for p in product)
        b_weight = (b_weight[0] / gamma, b_weight[1] / gamma)
        entries = (inverse, cmul(inverse, first), cmul(inverse, a_weight), cmul(inverse, b_weight))
        for e, (re, im) in enumerate(entries):
            table_ref[2 * e, m] = re
            table_ref[2 * e + 1, m] = im
    for k in range(phase_ref.shape[0]):
        for axis in range(2):
            angle = full(phase_ref[k : k + 1, axis : axis + 1])
            trig_ref[k, axis, 0] = jnp.cos(angle)
            trig_ref[k, axis, 1] = jnp.sin(angle)
    depth = chain_ref.shape[2]
    row = lax.broadcasted_iota(jnp.int32, shape, 0)
    tiles = [[], []]
    for c in range(2):
        for t in range(depth // SUB):
            value = zero
            for r in range(SUB):
                b = t * SUB + r
                if 1 <= b <= totals:
                    value = jnp.where(row == r, steps[b - 1][c], value)
            tiles[c].append(value)
    step = tuple(jnp.concatenate(tile, 0) for tile in tiles)
    for s in range(chain_ref.shape[0]):
        chain_ref[s, 0] = step[0]
        chain_ref[s, 1] = step[1]
        moved = (pltpu.roll(step[0], 1 << s, 0), pltpu.roll(step[1], 1 << s, 0))
        step = cmul(step, moved)


def spread_lanes(tiles):
    count = len(tiles)
    shape = tiles[0].shape
    lane = lax.broadcasted_iota(jnp.int32, shape, 1)
    owner = lane // (LANES // count)
    result = []
    for j in range(count):
        index = lax.rem(lane * count + j, LANES)
        value = jnp.take_along_axis(tiles[0], index, axis=1)
        for t in range(1, count):
            value = jnp.where(owner == t, jnp.take_along_axis(tiles[t], index, axis=1), value)
        result.append(value)
    return result


def spread(full_ref, own_ref):
    planes, tiles, rows, _ = own_ref.shape
    for plane in range(planes):
        for r in range(0, rows, SUB):
            values = spread_lanes([full_ref[plane, t, r : r + SUB, :] for t in range(tiles)])
            for j, value in enumerate(values):
                own_ref[plane, j, r : r + SUB, :] = value


def picker(label, table_ref):
    mats = table_ref.shape[1]
    picks = [label == float(m) for m in range(1, mats)]

    def pick(e):
        value = table_ref[e, 0]
        for m in range(1, mats):
            value = jnp.where(picks[m - 1], table_ref[e, m], value)
        return value

    return pick


def ends(axis):
    first = (lax.axis_index(axis) == 0).astype(F32)
    last = (lax.axis_index(axis) == lax.axis_size(axis) - 1).astype(F32)
    return first, last


def row_turns(trig_ref, k):
    first, last = ends("gx")
    low = lax.broadcasted_iota(jnp.int32, (2 * HALO, LANES), 0) < HALO
    edge = jnp.where(low, last, first) > 0.5
    sine = trig_ref[k, 0, 1][0:1, :]
    co = jnp.where(edge, trig_ref[k, 0, 0][0:1, :], 1.0)
    return co, jnp.where(edge, jnp.where(low, sine, -sine), 0.0)


def column_halo(near, far, trig_ref, planes):
    y_even = even("gy")
    right_src = jnp.where(y_even, near, far)
    left_src = jnp.where(y_even, far, near)
    lane = lax.broadcasted_iota(jnp.int32, near.shape, 1)
    is_right = lane < HALO
    is_left = lane >= LANES - HALO
    values = []
    for plane in range(planes):
        right = pltpu.roll(right_src, (LANES - plane * SLOT) % LANES, 1)
        left = pltpu.roll(left_src, (LANES - HALO - plane * SLOT) % LANES, 1)
        values.append(jnp.where(is_right, right, jnp.where(is_left, left, 0.0)))
    first, last = ends("gy")
    edge = jnp.where(is_right, last, jnp.where(is_left, first, 0.0)) > 0.5
    for k in range(planes // 2):
        sine = trig_ref[k, 1, 1][0:1, :]
        co = jnp.where(edge, trig_ref[k, 1, 0][0:1, :], 1.0)
        si = jnp.where(edge, jnp.where(is_right, sine, -sine), 0.0)
        values[2 * k : 2 * k + 2] = cmul(values[2 * k : 2 * k + 2], (co, si))
    return values


def stage(own_ref, near_x, far_x, near_y, far_y, table_ref, trig_ref,
          cell_ref, b_ref, side_ref, raw_ref, work_ref):
    planes, tiles, rows, _ = own_ref.shape
    points = planes // 2
    total = rows + 2 * HALO
    count = total // SUB
    x_even = even("gx")
    for plane in range(planes):
        span = slice(plane * HALO, (plane + 1) * HALO)
        for t in range(tiles):
            lanes = slice(t * LANES, (t + 1) * LANES)
            near = near_x[span, lanes]
            far = far_x[span, lanes]
            raw_ref[plane, t, 0:HALO, :] = jnp.where(x_even, near, far)
            raw_ref[plane, t, HALO : 2 * HALO, :] = jnp.where(x_even, far, near)
            work_ref[plane, t, 0:rows, :] = own_ref[plane, t]
    for k in range(points):
        turn = row_turns(trig_ref, k)
        for t in range(tiles):
            turned = cmul((raw_ref[2 * k, t], raw_ref[2 * k + 1, t]), turn)
            raw_ref[2 * k, t] = turned[0]
            raw_ref[2 * k + 1, t] = turned[1]
    for plane in range(planes):
        for r in range(0, 2 * HALO, SUB):
            values = spread_lanes([raw_ref[plane, t, r : r + SUB, :] for t in range(tiles)])
            for j, value in enumerate(values):
                work_ref[plane, j, rows + r : rows + r + SUB, :] = value
    for plane, value in enumerate(column_halo(near_y[...], far_y[...], trig_ref, planes)):
        side_ref[plane] = value
    for j in range(tiles):
        for v in range(count):
            span = pl.ds(v, SUB, stride=count)
            pick = picker(work_ref[planes - 1, j, span, :], table_ref)
            for n, e in enumerate((0, 1, 4, 5, 6, 7)):
                cell_ref[n, j, v] = pick(e)
            weight = (pick(2), pick(3))
            for k in range(points):
                z = (work_ref[2 * k, j, span, :], work_ref[2 * k + 1, j, span, :])
                for c, value in enumerate(cmul(weight, z)):
                    b_ref[k, c, j, v] = value


def solve(own_ref, side_ref, near_c, far_c, table_ref, trig_ref, cell_own, b_own,
          out_ref, gram_ref, halo_ref, cell_halo, b_ref, x_ref, w_ref, keep_ref):
    planes, tiles, rows, _ = own_ref.shape
    points = planes // 2
    total = rows + 2 * HALO
    count = total // SUB
    corner = column_halo(near_c[...], far_c[...], trig_ref, planes)
    for k in range(points):
        corner[2 * k : 2 * k + 2] = cmul(corner[2 * k : 2 * k + 2], row_turns(trig_ref, k))
    for plane in range(planes):
        halo_ref[plane, 0:rows, :] = side_ref[plane]
        halo_ref[plane, rows:total, :] = corner[plane]
    for v in range(count):
        span = pl.ds(v, SUB, stride=count)
        pick = picker(halo_ref[planes - 1, span, :], table_ref)
        for n, e in enumerate((0, 1, 4, 5, 6, 7)):
            cell_halo[n, v] = pick(e)
        weight = (pick(2), pick(3))
        for k in range(points):
            z = (halo_ref[2 * k, span, :], halo_ref[2 * k + 1, span, :])
            for c, value in enumerate(cmul(weight, z)):
                b_ref[k, c, tiles, v] = value

    def cell(e, t, v):
        return cell_own[e, t, v] if t < tiles else cell_halo[e, v]

    lane8 = lax.broadcasted_iota(jnp.int32, (SUB, LANES), 1)
    at_first = lane8 == 0
    at_last = lane8 == LANES - 1

    def sweep(src, right_side, dst_ref):
        held = {}
        for k, v in [(k, v) for v in range(count) for k in range(points)]:
                sums = []
                for c in range(2):
                    x = [src(k, c, t, v) for t in range(tiles + 1)]
                    last_on = pltpu.roll(x[tiles - 1], 1, 1)
                    halo_on = pltpu.roll(x[tiles], 1, 1)
                    first_back = pltpu.roll(x[0], LANES - 1, 1)
                    halo_back = pltpu.roll(x[tiles], LANES - 1, 1)
                    left = [jnp.where(at_first, halo_on, last_on)] + x[: tiles - 1]
                    right = x[1:tiles] + [jnp.where(at_last, halo_back, first_back)]
                    left.append(jnp.where(at_first, last_on, halo_on))
                    right.append(jnp.where(at_last, first_back, halo_back))
                    before = held.get((k, c))
                    after = []
                    total_n = []
                    for t in range(tiles + 1):
                        if v < count - 1:
                            down = src(k, c, t, v + 1)
                        else:
                            down = pltpu.roll(src(k, c, t, 0), SUB - 1, 0)
                        after.append(right[t] + down)
                        if before is not None and 0 < t < tiles:
                            other = before[t - 1]
                        elif v > 0:
                            other = left[t] + src(k, c, t, v - 1)
                        else:
                            other = left[t] + pltpu.roll(src(k, c, t, count - 1), 1, 0)
                        total_n.append(other + after[t])
                    held[k, c] = after
                    sums.append(total_n)
                for t in range(tiles + 1):
                    n = cmul((cell(0, t, v), cell(1, t, v)), (sums[0][t], sums[1][t]))
                    for c in range(2):
                        dst_ref[k, c, t, v] = right_side(k, c, t, v) + n[c]

    def reader(ref):
        return lambda *at: ref[at]

    def first_side(k, c, t, v):
        return b_own[k, c, t, v] if t < tiles else b_ref[k, c, t, v]

    for s in range(STEPS):
        right_side = reader(b_ref) if s else first_side
        sweep(right_side, right_side, w_ref)
        sweep(reader(w_ref), right_side, x_ref)
        for _ in range(SWEEPS // 2 - 1):
            sweep(reader(x_ref), right_side, w_ref)
            sweep(reader(w_ref), right_side, x_ref)
        for k in range(points):
            for t in range(tiles + 1):
                for v in range(count):
                    span = pl.ds(v, SUB, stride=count)
                    y = (x_ref[k, 0, t, v], x_ref[k, 1, t, v])
                    for c in range(2):
                        if t < tiles:
                            out_ref[s, k, c, t, span, :] = y[c]
                        elif s == 0:
                            keep_ref[k, c, v] = y[c]
                    if s < STEPS - 1:
                        b = cmul((cell(2, t, v), cell(3, t, v)), y)
                        if s == 1:
                            if t < tiles:
                                old = (out_ref[0, k, 0, t, span, :], out_ref[0, k, 1, t, span, :])
                            else:
                                old = (keep_ref[k, 0, v], keep_ref[k, 1, v])
                            b = cadd(b, cmul((cell(4, t, v), cell(5, t, v)), old))
                        for c in range(2):
                            b_ref[k, c, t, v] = b[c]

    names = STEPS + 1
    zero = jnp.zeros((SUB, LANES), F32)
    line = jnp.zeros((1, LANES), F32)
    lane1 = lax.broadcasted_iota(jnp.int32, (1, LANES), 1)
    entries = [(i, j) for i in range(names) for j in range(i, names)]
    for k in range(points):

        def gather(r, accs):
            accs = list(accs)
            span = pl.ds(pl.multiple_of(r * SUB, SUB), SUB)
            for t in range(tiles):
                fields = [(own_ref[2 * k, t, span, :], own_ref[2 * k + 1, t, span, :])]
                for s in range(STEPS):
                    fields.append((out_ref[s, k, 0, t, span, :], out_ref[s, k, 1, t, span, :]))
                at = 0
                for i, j in entries:
                    if i == j:
                        a = fields[i]
                        accs[at] = accs[at] + (a[0] * a[0] + a[1] * a[1])
                        at += 1
                    else:
                        product = conj_mul(fields[i], fields[j])
                        accs[at] = accs[at] + product[0]
                        accs[at + 1] = accs[at + 1] + product[1]
                        at += 2
            return tuple(accs)

        accs = lax.fori_loop(0, rows // SUB, gather, (zero,) * (names * names))
        for e, acc in enumerate(accs):
            value = jnp.sum(jnp.sum(acc, axis=0, keepdims=True), axis=1, keepdims=True)
            line = jnp.where(lane1 == k * names * names + e, value, line)
    gram_ref[...] = jnp.broadcast_to(line[None], gram_ref.shape)


def finish(own_ref, out_ref, part_ref, chain_ref, size_ref, basis_ref, hess_out,
           found_ref, turn_ref, done_ref, hess_ref, sem, hess_sem):
    planes, tiles, rows, _ = own_ref.shape
    points = planes // 2
    names = STEPS + 1
    shape = (SUB, LANES)
    line = jnp.sum(part_ref[:, 0, :], axis=0, keepdims=True)
    uppers = []
    inverses = []
    copies = []
    for k in range(points):
        base = k * names * names
        gram = {}
        at = base
        for i in range(names):
            for j in range(i, names):
                width = 1 if i == j else 2
                gram[i, j] = tuple(
                    jnp.broadcast_to(line[:, at + c : at + c + 1], shape) for c in range(width)
                )
                at += width
        upper = {}
        inv = []
        for i in range(names):
            pivot = gram[i, i][0]
            for l in range(i):
                pivot = pivot - (upper[l, i][0] * upper[l, i][0] + upper[l, i][1] * upper[l, i][1])
            root = jnp.sqrt(pivot)
            upper[i, i] = root
            inv.append(1.0 / root)
            for j in range(i + 1, names):
                value = gram[i, j]
                for l in range(i):
                    value = csub(value, conj_mul(upper[l, i], upper[l, j]))
                upper[i, j] = (value[0] * inv[i], value[1] * inv[i])
        uppers.append(upper)
        inverses.append(inv)

    def combine(k, r):
        upper = uppers[k]
        inv = inverses[k]
        span = slice(r * SUB, (r + 1) * SUB)
        for t in range(tiles):
            fields = [(own_ref[2 * k, t, span, :], own_ref[2 * k + 1, t, span, :])]
            for s in range(STEPS):
                fields.append((out_ref[s, k, 0, t, span, :], out_ref[s, k, 1, t, span, :]))
            found = []
            for i in range(names):
                value = fields[i]
                for l in range(i):
                    value = csub(value, cmul(upper[l, i], found[l]))
                value = (value[0] * inv[i], value[1] * inv[i])
                found.append(value)
                if i > 0:
                    for c in range(2):
                        place = slice(c * rows + r * SUB, c * rows + (r + 1) * SUB)
                        found_ref[k, i - 1, t, place, :] = value[c]

    piece = 32
    for k in range(points):
        for r in range(rows // SUB):
            combine(k, r)
        for i in range(STEPS):
            for n in range(0, 2 * rows, LANES):
                for t in range(tiles):
                    turned = found_ref[k, i, t, n : n + LANES, :].T
                    turn_ref[k, i, pl.ds(t, LANES, stride=tiles), :] = turned
                for t in range(tiles):
                    lanes = slice(t * LANES, (t + 1) * LANES)
                    done_ref[k, i, n : n + LANES, lanes] = turn_ref[k, i, lanes, :].T
            for at, n in enumerate(range(0, 2 * rows, piece)):
                part = pl.ds(n, piece)
                copy = pltpu.make_async_copy(
                    done_ref.at[k, i, part, :], basis_ref.at[k, i, part, :], sem.at[k, i, at]
                )
                copy.start()
                copies.append(copy)

    lane = lax.broadcasted_iota(jnp.int32, shape, 1)

    def mixed(pick):
        value = pick(0)
        for k in range(1, points):
            value = jnp.where(lane == k, pick(k), value)
        return value

    gamma = size_ref[...]
    inv0 = mixed(lambda k: inverses[k][0])
    column = []
    for j in range(1, names):
        entry = []
        for i in range(j):
            entry.append(tuple(mixed(lambda k: uppers[k][i, j][c]) * inv0 for c in range(2)))
        entry.append((mixed(lambda k: uppers[k][j, j]) * inv0, jnp.zeros(shape, F32)))
        column.append(entry)

    depth = chain_ref.shape[2]
    row = lax.broadcasted_iota(jnp.int32, (depth, LANES), 0)
    tall = lambda value: jnp.broadcast_to(value[0:1], (depth, LANES))
    nil = jnp.zeros((depth, LANES), F32)
    at_top = row == 0
    basis_u = [[(jnp.where(at_top, 1.0, 0.0), nil)]]
    hess = {}
    coords = []
    mus = []
    for k in range(STEPS):
        active = k + 1
        if k == 0:
            found = column[0]
        elif k == 1:
            found = []
            for i in range(3):
                value = (column[1][i][0] * gamma, column[1][i][1] * gamma)
                if i < 2:
                    value = csub(value, cmul(hess[0, 0], coords[0][i]))
                found.append((value[0] / mus[0], value[1] / mus[0]))
        else:
            found = []
            scale = gamma / mus[0]
            for i in range(4):
                value = (column[2][i][0] * gamma, column[2][i][1] * gamma)
                if i < 3:
                    value = csub(value, cmul(hess[0, 0], column[1][i]))
                value = (value[0] * scale, value[1] * scale)
                if i < 2:
                    value = csub(value, cmul(hess[0, 1], coords[0][i]))
                if i < 3:
                    value = csub(value, cmul(hess[1, 1], coords[1][i]))
                found.append((value[0] / mus[1], value[1] / mus[1]))
        coords.append(found)
        current = basis_u[k]
        x = []
        for i in range(active + 1):
            old = current[i] if i < len(current) else (nil, nil)
            value = tuple(jnp.where(at_top, tall(found[i][c]), old[c]) for c in range(2))
            for s in range(chain_ref.shape[0]):
                step = (chain_ref[s, 0], chain_ref[s, 1])
                moved = tuple(pltpu.roll(value[c], 1 << s, 0) for c in range(2))
                value = cadd(value, cmul(step, moved))
            x.append(value)
        total_t = [None] * active
        for turn in range(2):
            inner = []
            for j in range(active):
                acc = (nil, nil)
                for i in range(len(basis_u[j])):
                    acc = cadd(acc, conj_mul(basis_u[j][i], x[i]))
                inner.append(tuple(jnp.sum(acc[c], axis=0, keepdims=True) for c in range(2)))
            for j in range(active):
                for i in range(len(basis_u[j])):
                    x[i] = csub(x[i], cmul(inner[j], basis_u[j][i]))
                total_t[j] = inner[j] if turn == 0 else cadd(total_t[j], inner[j])
        square = nil
        for value in x:
            square = square + (value[0] * value[0] + value[1] * value[1])
        mu = jnp.sqrt(jnp.sum(square, axis=0, keepdims=True))
        mus.append(jnp.broadcast_to(mu, shape))
        basis_u.append([(value[0] / mu, value[1] / mu) for value in x])
        for j in range(active):
            hess[j, k] = tuple(jnp.broadcast_to(total_t[j][c], shape) for c in range(2))
    part_row = lax.broadcasted_iota(jnp.int32, (2, names), 0)
    part_lane = lax.broadcasted_iota(jnp.int32, (2, names), 1)
    for p in range(points):
        for k in range(STEPS):
            value = jnp.zeros((2, names), F32)
            for j in range(k + 2):
                parts = hess[j, k] if j <= k else (mus[k],)
                for c, entry in enumerate(parts):
                    here = (part_row == c) & (part_lane == j)
                    value = jnp.where(here, entry[0:1, p : p + 1], value)
            hess_ref[p, k] = value
    copy = pltpu.make_async_copy(hess_ref, hess_out, hess_sem)
    copy.start()
    copies.append(copy)
    for copy in copies:
        copy.wait()


def call(body, outs, specs, out_specs, scratch=(), limit=16):
    return pl.pallas_call(
        body,
        out_shape=outs,
        in_specs=specs,
        out_specs=out_specs,
        scratch_shapes=list(scratch),
        compiler_params=pltpu.CompilerParams(vmem_limit_bytes=limit * MIB),
    )


def per_device(
    initial_guess_field,
    medium_label,
    principal_entry_addend,
    linearized_block_weight,
    sample_abscissae,
    singularity_locations,
    basis_normalizers,
    spectral_target,
    quasi_periodic_phase,
):
    points, _, rows, columns = initial_guess_field.shape
    blocks, mats, _ = linearized_block_weight.shape
    tiles = columns // LANES
    planes = 2 * points + 1
    total = rows + 2 * HALO
    count = total // SUB
    names = STEPS + 1
    depth = -(-blocks // SUB) * SUB
    levels = (blocks - 1).bit_length()
    devices = lax.axis_size("gx") * lax.axis_size("gy")
    sds = lambda *shape: jax.ShapeDtypeStruct(shape, F32)

    packed = -(-planes * HALO // SUB) * SUB
    small = [
        principal_entry_addend.T,
        linearized_block_weight.transpose(1, 2, 0),
        sample_abscissae.T,
        singularity_locations.T,
        basis_normalizers.reshape(1, -1),
        spectral_target.reshape(1, -1),
        quasi_periodic_phase,
    ]
    hbm = lambda v: pltpu.with_memory_space_constraint(v, pltpu.HBM)
    field = hbm(initial_guess_field)
    label = hbm(medium_label)
    near_x, far_x = call(
        pack_rows,
        [sds(packed, columns)] * 2,
        [HBM] * 2,
        [VMEM] * 2,
        [
            pltpu.VMEM((2 * points, 2, STRIP, columns), F32),
            pltpu.VMEM((2, STRIP, columns), jnp.int32),
            pltpu.SemaphoreType.DMA((2 * planes,)),
        ],
        limit=8,
    )(field, label)

    def send(value, axis, pairs):
        return lax.ppermute(value, axis, pairs(axis))

    far_x = send(far_x, "gx", swap_far)
    near_x = send(near_x, "gx", swap_near)
    full, near_y, far_y, *small = call(
        load,
        [sds(planes, tiles, rows, LANES)]
        + [sds(rows, LANES)] * 2
        + [sds(*value.shape) for value in small],
        [HBM] * 9,
        [VMEM] * 10,
        [
            pltpu.VMEM((tiles, rows, LANES), jnp.int32),
            pltpu.SemaphoreType.DMA((tiles * planes + len(small),)),
        ],
        limit=8,
    )(field, label, *[hbm(v) for v in small])
    far_y = send(far_y, "gy", swap_far)
    near_y = send(near_y, "gy", swap_near)

    table, trig, chain, size = call(
        params,
        [
            sds(8, mats, SUB, LANES),
            sds(points, 2, 2, SUB, LANES),
            sds(levels, 2, depth, LANES),
            sds(SUB, LANES),
        ],
        [VMEM] * 7,
        [VMEM] * 4,
        limit=4,
    )(*small)

    own = call(spread, sds(planes, tiles, rows, LANES), [VMEM], VMEM, limit=4)(full)

    near_c, far_c = call(
        pack_corners,
        [sds(2 * HALO, LANES)] * 2,
        [VMEM] * 2,
        [VMEM] * 2,
        [pltpu.VMEM((planes, 2, 2 * HALO, LANES), F32)],
        limit=4,
    )(near_x, far_x)
    far_c = send(far_c, "gy", swap_far)
    near_c = send(near_c, "gy", swap_near)

    narrow = (tiles, count, SUB, LANES)
    cell, b, side = call(
        stage,
        [sds(6, *narrow), sds(points, 2, *narrow), sds(planes, rows, LANES)],
        [VMEM] * 7,
        [VMEM] * 3,
        [
            pltpu.VMEM((planes, tiles, 2 * HALO, LANES), F32),
            pltpu.VMEM((planes, tiles, total, LANES), F32),
        ],
        limit=8,
    )(own, near_x, far_x, near_y, far_y, table, trig)

    wide = (tiles + 1, count, SUB, LANES)
    out, gram = call(
        solve,
        [sds(STEPS, points, 2, tiles, total, LANES), sds(devices, 1, LANES)],
        [VMEM] * 8,
        [VMEM] * 2,
        [
            pltpu.VMEM((planes, total, LANES), F32),
            pltpu.VMEM((6,) + wide[1:], F32),
        ]
        + [pltpu.VMEM((points, 2) + wide, F32)] * 3
        + [pltpu.VMEM((points, 2) + wide[1:], F32)],
        limit=32,
    )(own, side, near_c, far_c, table, trig, cell, b)

    part = lax.all_to_all(gram, ("gx", "gy"), 0, 0, tiled=True)

    basis, hess = call(
        finish,
        [sds(points, STEPS, 2 * rows, columns), sds(points, STEPS, 2, names)],
        [VMEM] * 5,
        [ANY, ANY],
        [
            pltpu.VMEM((points, STEPS, tiles, 2 * rows, LANES), F32),
            pltpu.VMEM((points, STEPS, columns, LANES), F32),
            pltpu.VMEM((points, STEPS, 2 * rows, columns), F32),
            pltpu.VMEM((points, STEPS, 2, names), F32),
            pltpu.SemaphoreType.DMA((points, STEPS, 2 * rows // 32)),
            pltpu.SemaphoreType.DMA,
        ],
        limit=16,
    )(own, out, part, chain, size)
    basis = basis.reshape(points, STEPS, 2, rows, columns)
    return basis, hess.transpose(0, 2, 3, 1)


def solution(mesh):
    return jax.shard_map(
        per_device,
        mesh=mesh,
        in_specs=(P(None, None, "gx", "gy"), P("gx", "gy"), P(), P(), P(), P(), P(), P(), P()),
        out_specs=(P(None, None, None, "gx", "gy"), P()),
        check_vma=False,
    )
```
